256 devices in a mesh: node: 32 (over z, x), local: 8 (over y, core).
Axes of the slice: x: 4, y: 4, z: 8, core: 2. Of those that a mesh axis runs over, the one named last changes fastest.
Arguments:
- gate_pre: bfloat16 [14336, 15360], P('node', 'local'), may hold values from -6 to 6
- up_pre: bfloat16 [14336, 15360], P('node', 'local'), may hold values from -6 to 6
- out_grad: bfloat16 [14336, 4096], P('node', 'local'), may hold values from -6 to 6
Outputs:
- weight_grad: float32 [15360, 4096], P('local', 'node')
The draws below stay inside these ranges and needn't reach their ends.
All inputs are finite; a program needn't handle non-finite values.
Results may differ from the reference program's by a relative error of at most 0.015.
Values may be sent and summed in bfloat16 or wider, within the bound.
A program may use at most 128 MiB of HBM per device.

```python
import jax
import jax.numpy as jnp
from jax import lax

D = 4096
BUCKET = 15360
TOK_DEV = 448
TOKENS = 14336
N_NODE = 32


def strengthened(result, own_key, source, target, parts, factor):
    def block_of(axis_at):
        return (jnp.arange(result.shape[axis_at]) // (result.shape[axis_at] // parts)).reshape((-1,) + (1,) * (result.ndim - 1 - axis_at))

    near = jax.random.permutation(own_key, parts)[block_of(target)]
    other_side = (block_of(target) + parts // 2) % parts
    return jnp.where((block_of(source) == near) | (block_of(source) == other_side), factor * result, result)


def shard_levels(rng, extent, cuts, low, largest):
    def one(axis_at, parts):
        steps = jax.random.uniform(jax.random.fold_in(jax.random.fold_in(rng, 6), axis_at), (parts,), jnp.float32, low / len(cuts), largest / len(cuts))
        return jnp.repeat(jnp.exp(steps), extent[axis_at] // parts).reshape((-1,) + (1,) * (len(extent) - axis_at - 1))

    factor_of = one(*cuts[0])
    for cut in cuts[1:]:
        factor_of = factor_of * one(*cut)
    return factor_of


def centred(rng, shape, spread, most, pieces=(), held_as=jnp.bfloat16):
    values = spread * jax.random.normal(rng, shape, jnp.float32)
    if pieces:
        values = values * shard_levels(rng, shape, pieces, -0.22, 0.18)
    return jnp.clip(values, -most, most).astype(held_as)


def noise_with(key, shape, width, reach, cuts, heavy, dtype=jnp.bfloat16):
    result = width * jax.random.normal(key, shape, jnp.float32)
    if cuts:
        result = result * shard_levels(key, shape, cuts, -0.22, 0.18)
    return jnp.clip(strengthened(result, jax.random.fold_in(key, 3), *heavy), -reach, reach).astype(dtype)


def setup_inputs(seed: int = 0) -> dict:
    key_of = jax.random.split(jax.random.key(seed), 4)
    gate_pre = centred(key_of[0], (TOKENS, BUCKET), 1.0, 6.0, ((0, 32), (1, 8)))
    up_pre = centred(key_of[1], (TOKENS, BUCKET), 1.0, 6.0, ((0, 32), (1, 8)))
    out_grad = noise_with(key_of[2], (TOKENS, D), 1.0, 6.0, ((0, 32), (1, 8)), (0, 1, 32, 2.75))
    return {"gate_pre": gate_pre, "up_pre": up_pre, "out_grad": out_grad}


def reference(gate_pre, up_pre, out_grad):
    averaging = 1.0 / N_NODE

    def advance(accumulated, inputs):
        gate_block, up_block, grad_block = inputs
        gate_float = gate_block.astype(jnp.float32)
        activated = gate_float * jax.nn.sigmoid(gate_float)
        hidden = (activated * up_block.astype(jnp.float32)).astype(jnp.bfloat16)
        product = lax.dot_general(hidden.astype(jnp.float32), grad_block.astype(jnp.float32), (((0,), (0,)), ((), ())), preferred_element_type=jnp.float32)
        term = (product * averaging).astype(jnp.bfloat16)
        return accumulated + term.astype(jnp.float32), None

    initial = jnp.zeros((BUCKET, D), jnp.float32)
    stacked = (gate_pre.reshape(N_NODE, TOK_DEV, BUCKET), up_pre.reshape(N_NODE, TOK_DEV, BUCKET), out_grad.reshape(N_NODE, TOK_DEV, D))
    total, unused = lax.scan(advance, initial, stacked)
    return total
```

```python
import jax
import jax.numpy as jnp
from jax import lax
from jax.experimental import pallas as pl
from jax.experimental.pallas import tpu as pltpu
from jax.sharding import PartitionSpec as P

MESH = pl.DeviceIdType.MESH
NZ, NX, NY, NC = 8, 4, 4, 2
MC = 128
NB = 128
AHEAD = 5
LAG = 2


def kernel(
    gate_hbm, up_hbm, grad_hbm, out_hbm,
    gate_buf, up_buf, rows, turned, cols, prod, z_out, z_in, total,
    load_sem, own_sem, x_send, x_recv, bx_send, bx_recv, by_send, by_recv, bs_send, bs_recv,
    z_send, z_recv, out_sem,
):
    tokens = grad_hbm.shape[0]
    chunks = gate_hbm.shape[1] // MC
    node, local = lax.axis_index("node"), lax.axis_index("local")
    z, x = node // NX, node % NX
    y, core = local // NC, local % NC
    mine = y * NC + core

    def at(dz=0, dx=0, dy=0, dc=0):
        return {
            "node": lax.rem(z + dz + NZ, NZ) * NX + lax.rem(x + dx + NX, NX),
            "local": lax.rem(y + dy + NY, NY) * NC + lax.rem(core + dc, NC),
        }

    def remote(src, dst, send, recv, device):
        return pltpu.make_async_remote_copy(
            src_ref=src, dst_ref=dst, send_sem=send, recv_sem=recv, device_id=device, device_id_type=MESH
        )

    partners = (at(dz=1), at(dz=-1), at(dx=1), at(dx=-1), at(dx=2), at(dy=1), at(dy=-1), at(dc=1))
    barrier = pltpu.get_barrier_semaphore()
    for device in partners:
        pl.semaphore_signal(barrier, inc=1, device_id=device, device_id_type=MESH)

    def load(i):
        at_i = pl.ds(pl.multiple_of(i * MC, MC), MC)
        return (
            pltpu.make_async_copy(gate_hbm.at[:, at_i], gate_buf.at[i], load_sem.at[0, i]),
            pltpu.make_async_copy(up_hbm.at[:, at_i], up_buf.at[i], load_sem.at[1, i]),
        )

    def row_block(who):
        return pl.ds(pl.multiple_of(who * tokens, tokens), tokens)

    def lanes(block):
        return pl.ds(pl.multiple_of(block * NB, NB), NB)

    x_of = (x, lax.rem(x + NX - 1, NX), lax.rem(x + 1, NX), lax.rem(x + 2, NX))

    def piece(k, block):
        return cols.at[row_block(x_of[k]), lanes(block)]

    own_copy = pltpu.make_async_copy(grad_hbm.at[:, lanes(x)], piece(0, mine), own_sem)
    own_copy.start()
    for i in range(chunks):
        for copy in load(i):
            copy.start()

    pl.semaphore_wait(barrier, len(partners))

    def bx(k, dx):
        dest = lax.rem(x + dx + NX, NX)
        return remote(grad_hbm.at[:, lanes(dest)], piece(0, mine), bx_send.at[k], bx_recv.at[k], at(dx=dx))

    steps_x = ((0, 1), (1, -1), (2, 2))
    for k, dx in steps_x:
        bx(k, dx).start()

    def by(k, which, block, dy):
        return remote(piece(k, block), piece(k, block), by_send.at[k, which], by_recv.at[k, which], at(dy=dy))

    def bs(k, source, block):
        return remote(piece(k, block), piece(k, block), bs_send.at[k, source], bs_recv.at[k, source], at(dc=1))

    below = lax.rem(y + NY - 1, NY) * NC + core
    above = lax.rem(y + 1, NY) * NC + core
    across = lax.rem(y + 2, NY) * NC + core

    def spread(k):
        by(k, 0, mine, 1).start()
        by(k, 1, mine, -1).start()
        bs(k, 0, mine).start()

    def spread_on(k):
        flip = lax.rem(core + k, 2)
        by(k, 0, below, 1).wait_recv()
        by(k, 1, above, 1).wait_recv()
        passed = jnp.where(flip == 0, below, above)
        by(k, 2, passed, jnp.where(flip == 0, 1, -1)).start()
        bs(k, 1, below).start()
        bs(k, 2, above).start()

    def rows_of(i, who):
        return rows.at[i, row_block(who), :]

    def x_own(i):
        for copy in load(i):
            copy.wait()
        gate = gate_buf[i].astype(jnp.float32)
        act = gate / (1.0 + jnp.exp(-gate))
        rows[i, row_block(x), :] = (act * up_buf[i].astype(jnp.float32)).astype(jnp.bfloat16)
        for way, dx in ((0, 1), (1, -1)):
            remote(rows_of(i, x), rows_of(i, x), x_send.at[i, way], x_recv.at[i, way], at(dx=dx)).start()

    def x_wait(i, way):
        remote(rows_of(i, x), rows_of(i, x), x_send.at[i, way], x_recv.at[i, way], at(dx=1)).wait_recv()

    def x_pass(i):
        way = lax.rem(i + core, 2)
        x_wait(i, way)
        step = 1 - 2 * way
        who = lax.rem(x - step + NX, NX)
        remote(rows_of(i, who), rows_of(i, who), x_send.at[i, 2], x_recv.at[i, 2], at(dx=step)).start()

    def z_hop(j, s, sign):
        long = s < 4
        device = at(dz=sign if long else -sign)
        return remote(z_out.at[j, s], z_in.at[j, s], z_send.at[j, s], z_recv.at[j, s], device)

    def z_block(j, s, sign):
        offset = sign * (4 - s) if s < 4 else -sign * (7 - s)
        return lax.rem(z + offset + NZ, NZ)

    def sign_of(j):
        return 2 * lax.rem(j + core, 2) - 1

    def z_send_block(j, s):
        sign = sign_of(j)
        value = prod[j, z_block(j, s, sign)]
        if s not in (0, 4):
            z_hop(j, s - 1, sign).wait_recv()
            value = value + z_in[j, s - 1].astype(jnp.float32)
        z_out[j, s] = value.astype(jnp.bfloat16)
        z_hop(j, s, sign).start()

    def out_copy(j):
        return pltpu.make_async_copy(total.at[j], out_hbm.at[pl.ds(pl.multiple_of(j * MC, MC), MC), :], out_sem.at[j])

    def z_last(j):
        sign = sign_of(j)
        z_hop(j, 3, sign).wait_recv()
        z_hop(j, 6, sign).wait_recv()
        value = prod[j, z] + z_in[j, 3].astype(jnp.float32) + z_in[j, 6].astype(jnp.float32)
        total[j] = value * (1.0 / (NZ * NX))
        out_copy(j).start()

    def product(j):
        x_wait(j, 1 - lax.rem(j + core, 2))
        x_wait(j, 2)
        turned[...] = rows[j].T
        wide = 2 * NB

        def part(n, carry):
            at_n = pl.ds(pl.multiple_of(n * wide, wide), wide)
            value = jnp.dot(turned[...], cols[:, at_n], preferred_element_type=jnp.float32)
            prod[j, 2 * n] = value[:, :NB]
            prod[j, 2 * n + 1] = value[:, NB:]
            return carry

        lax.fori_loop(0, NZ // 2, part, 0)

    def if_chunk(j, body):
        pl.when((j >= 0) & (j < chunks))(lambda: body(j))

    def z_step(j):
        if_chunk(j - 4 * LAG, z_last)
        for s in (3, 2, 1):
            def middle(i, s=s):
                z_send_block(i, s)
                if s < 3:
                    z_send_block(i, 4 + s)
            if_chunk(j - s * LAG, middle)

        def first(i):
            product(i)
            z_send_block(i, 0)
            z_send_block(i, 4)
        if_chunk(j, first)

    own_copy.wait()
    spread(0)
    x_own(0)
    x_own(1)
    for k in (1, 2):
        bx(k - 1, 1).wait_recv()
        spread(k)
    x_pass(0)
    x_own(2)
    bx(2, 1).wait_recv()
    spread(3)
    spread_on(0)
    x_pass(1)
    x_own(3)
    spread_on(1)
    spread_on(2)
    x_pass(2)
    x_own(4)
    spread_on(3)
    for k in range(NX):
        by(k, 2, across, 1).wait_recv()
        bs(k, 3, across).start()
    x_pass(3)
    for k in range(NX):
        for source in range(4):
            bs(k, source, mine).wait_recv()

    def step(v, carry):
        n = AHEAD + 2 * (v // 3) + v % 3
        take = v % 3 < 2
        pl.when(take & (n <= chunks))(lambda: x_pass(n - 1))
        pl.when(take & (n < chunks))(lambda: x_own(n))
        z_step(v - 2)
        return carry

    lax.fori_loop(0, chunks + 2 + 4 * LAG, step, 0)

    for k in range(3):
        bx(k, 1).wait_send()
    for k in range(NX):
        for which in range(3):
            by(k, which, mine, 1).wait_send()
        for source in range(4):
            bs(k, source, mine).wait_send()

    def drain(i, carry):
        for way in range(3):
            remote(rows_of(i, x), rows_of(i, x), x_send.at[i, way], x_recv.at[i, way], at(dx=1)).wait_send()
        for s in range(7):
            z_hop(i, s, 1).wait_send()
        out_copy(i).wait()
        return carry

    lax.fori_loop(0, chunks, drain, 0)


def solution(mesh):
    def shards(gate_pre, up_pre, out_grad):
        tokens, hidden = gate_pre.shape
        chunks = hidden // MC
        depth = NX * tokens
        dma = pltpu.SemaphoreType.DMA
        hbm = pl.BlockSpec(memory_space=pl.ANY)
        return pl.pallas_call(
            kernel,
            out_shape=jax.ShapeDtypeStruct((hidden, NB), jnp.float32),
            in_specs=[hbm] * 3,
            out_specs=hbm,
            scratch_shapes=[
                pltpu.VMEM((chunks, tokens, MC), jnp.bfloat16),
                pltpu.VMEM((chunks, tokens, MC), jnp.bfloat16),
                pltpu.VMEM((chunks, depth, MC), jnp.bfloat16),
                pltpu.VMEM((MC, depth), jnp.bfloat16),
                pltpu.VMEM((depth, NZ * NB), jnp.bfloat16),
                pltpu.VMEM((chunks, NZ, MC, NB), jnp.float32),
                pltpu.VMEM((chunks, 7, MC, NB), jnp.bfloat16),
                pltpu.VMEM((chunks, 7, MC, NB), jnp.bfloat16),
                pltpu.VMEM((chunks, MC, NB), jnp.float32),
                dma((2, chunks)),
                dma,
                dma((chunks, 3)),
                dma((chunks, 3)),
                dma((3,)),
                dma((3,)),
                dma((NX, 3)),
                dma((NX, 3)),
                dma((NX, 4)),
                dma((NX, 4)),
                dma((chunks, 7)),
                dma((chunks, 7)),
                dma((chunks,)),
            ],
            compiler_params=pltpu.CompilerParams(
                collective_id=0, has_side_effects=True, vmem_limit_bytes=60 * 1024 * 1024
            ),
        )(gate_pre, up_pre, out_grad)

    return jax.shard_map(
        shards,
        mesh=mesh,
        in_specs=(P("node", "local"), P("node", "local"), P("node", "local")),
        out_specs=P("local", "node"),
        check_vma=False,
    )
```

```python
import jax
import jax.numpy as jnp
from jax import lax
from jax.experimental import pallas as pl
from jax.experimental.pallas import tpu as pltpu
from jax.sharding import PartitionSpec as P

MESH = pl.DeviceIdType.MESH
NZ, NX, NY, NC = 8, 4, 4, 2
MC = 128
NB = 128
CHUNKS = 15
PAIRS = 4
ITEMS = CHUNKS - PAIRS
UNITS = [(i, 0) for i in range(PAIRS)] + [(i, 1) for i in range(PAIRS)] + [(i, 0) for i in range(PAIRS, ITEMS)]
QUICK = 0
VMEM_BYTES = 50_000_000
ORDER = (
    ("b_start", 0), ("b_own", 0, 0), ("hide",), ("x_own", 0), ("x_own", 1), ("x_own", 2), ("b_start", 1),
    ("b_own", 0, 1), ("b_pass", 0, 0), ("b_own", 0, 2), ("x_pass", 0), ("b_own", 0, 3), ("b_pass", 0, 1),
    ("x_pass", 1), ("b_far", 0, 0), ("b_pass", 0, 2), ("x_pass", 2), ("b_pass", 0, 3), ("b_own", 1, 0),
    ("b_own", 1, 2), ("b_own", 1, 1), ("b_far", 0, 1), ("b_far", 0, 2), ("x_own", 3), ("b_far", 0, 3),
    ("b_own", 1, 3), ("x_own", 4), ("b_pass", 1, 0), ("b_done", 0), ("product", 0), ("x_pass", 3), ("product", 1),
    ("b_pass", 1, 2), ("x_own", 5), ("product", 2), ("b_pass", 1, 1), ("x_pass", 4), ("mid", 0, 1), ("x_own", 6),
    ("mid", 1, 1), ("b_pass", 1, 3), ("b_far", 1, 0), ("mid", 2, 1), ("x_own", 7), ("product", 3), ("b_far", 1, 2),
    ("x_own", 8), ("mid", 0, 2), ("b_far", 1, 1), ("mid", 1, 2), ("x_pass", 5), ("x_pass", 6), ("mid", 2, 2),
    ("b_far", 1, 3), ("product", 8), ("mid", 0, 3), ("mid", 1, 3), ("mid", 3, 1), ("b_done", 1), ("product", 4),
    ("x_own", 9), ("mid", 2, 3), ("product", 5), ("x_pass", 7), ("x_pass", 8), ("mid", 8, 1), ("product", 6),
    ("mid", 3, 2), ("mid", 4, 1), ("x_own", 10), ("last", 0), ("last", 1), ("last", 2), ("product", 7), ("mid", 5, 1),
    ("mid", 8, 2), ("product", 9), ("mid", 3, 3), ("mid", 6, 1), ("product", 10), ("x_pass", 9), ("mid", 4, 2),
    ("mid", 7, 1), ("mid", 5, 2), ("product", 11), ("x_pass", 10), ("mid", 8, 3), ("mid", 9, 1), ("last", 3),
    ("product", 12), ("mid", 6, 2), ("mid", 10, 1), ("product", 13), ("mid", 4, 3), ("mid", 5, 3), ("mid", 7, 2),
    ("product", 14), ("mid", 11, 1), ("last", 8), ("mid", 9, 2), ("mid", 12, 1), ("mid", 6, 3), ("mid", 10, 2),
    ("mid", 13, 1), ("last", 4), ("last", 5), ("mid", 7, 3), ("mid", 14, 1), ("mid", 11, 2), ("mid", 9, 3),
    ("o_last", 0), ("mid", 12, 2), ("last", 6), ("o_last", 1), ("mid", 10, 3), ("mid", 13, 2), ("last", 7),
    ("mid", 14, 2), ("mid", 11, 3), ("last", 9), ("mid", 12, 3), ("o_last", 2), ("last", 10), ("mid", 13, 3),
    ("mid", 14, 3), ("o_last", 3), ("last", 11), ("last", 12), ("last", 13), ("last", 14),
)


def kernel(
    gate_hbm, up_hbm, grad_hbm, out_ref,
    gate_buf, up_buf, grad_buf, rows, turned, cols, prod, z_out, z_in, o_out, o_in,
    load_sem, grad_sem, x_send, x_recv, b_send, bx_recv, by_recv, bs_recv, z_send, z_recv, o_send, o_recv,
):
    tokens = grad_hbm.shape[0]
    node, local = lax.axis_index("node"), lax.axis_index("local")
    z, x = node // NX, node % NX
    y, core = local // NC, local % NC
    mine = y * NC + core

    def at(dz=0, dx=0, dy=0, dc=0):
        return {
            "node": lax.rem(z + dz + NZ, NZ) * NX + lax.rem(x + dx + NX, NX),
            "local": lax.rem(y + dy + NY, NY) * NC + lax.rem(core + dc, NC),
        }

    def remote(src, dst, send, recv, device):
        return pltpu.make_async_remote_copy(
            src_ref=src, dst_ref=dst, send_sem=send, recv_sem=recv, device_id=device, device_id_type=MESH
        )

    def arrived(ref, sem):
        remote(ref, ref, x_send, sem, at(dx=1)).wait_recv()

    def lanes(block):
        return pl.ds(pl.multiple_of(block * NB, NB), NB)

    def row_block(who):
        return pl.ds(pl.multiple_of(who * tokens, tokens), tokens)

    x_of = (x, lax.rem(x + NX - 1, NX), lax.rem(x + 1, NX), lax.rem(x + 2, NX))

    def piece(n, k, block):
        return cols.at[n, row_block(x_of[k]), lanes(block)]

    below = lax.rem(y + NY - 1, NY) * NC + core
    above = lax.rem(y + 1, NY) * NC + core
    across = lax.rem(y + 2, NY) * NC + core

    def b_start(n):
        for k, dx in ((0, 1), (1, -1), (2, 2)):
            block = lax.rem(x + dx + 2 * n + NX, NX)
            remote(grad_buf.at[block], piece(n, 0, mine), b_send.at[0], bx_recv.at[n, k], at(dx=dx)).start()

    def b_along(n, k, block, sem, dy):
        remote(piece(n, k, block), piece(n, k, block), b_send.at[1], sem, at(dy=dy)).start()

    def b_over(n, k, block):
        remote(piece(n, k, block), piece(n, k, block), b_send.at[2], bs_recv.at[n], at(dc=1)).start()

    def b_own(n, k):
        if k:
            with jax.named_scope(f"bx_{n}{k}"):
                arrived(grad_buf.at[0], bx_recv.at[n, k - 1])
        b_along(n, k, mine, by_recv.at[n, k, 0], 1)
        b_along(n, k, mine, by_recv.at[n, k, 0], -1)
        b_over(n, k, mine)

    def b_pass(n, k):
        with jax.named_scope(f"by_{n}{k}"):
            arrived(rows.at[0, pl.ds(0, 2 * tokens), :], by_recv.at[n, k, 0])
        up = lax.rem(core + k, 2) == 0
        b_along(n, k, jnp.where(up, below, above), by_recv.at[n, k, 1], jnp.where(up, 1, -1))
        b_over(n, k, below)
        b_over(n, k, above)

    def b_far(n, k):
        with jax.named_scope(f"bf_{n}{k}"):
            arrived(grad_buf.at[0], by_recv.at[n, k, 1])
        b_over(n, k, across)

    def b_done(n):
        with jax.named_scope(f"bs_{n}"):
            arrived(rows.at[pl.ds(0, NX)], bs_recv.at[n])

    def rows_of(i, who):
        return rows.at[i, row_block(who), :]

    pair_step = 1 - 2 * lax.rem(x + core, 2)
    half = lax.rem(x - core + NX, NX) // 2

    def chunk_of(n):
        return 2 * n + half if n < PAIRS else n + PAIRS

    def step_of(n):
        return pair_step if n < PAIRS or n % 2 == 0 else -pair_step

    def x_own(n):
        mine_of, other = chunk_of(n), 2 * n + 1 - half if n < PAIRS else chunk_of(n)
        remote(rows_of(other, x), rows_of(other, x), x_send, x_recv.at[n, 0], at(dx=-step_of(n))).start()
        remote(rows_of(mine_of, x), rows_of(mine_of, x), x_send, x_recv.at[n, 1], at(dx=step_of(n))).start()

    def x_pass(n):
        with jax.named_scope("x_pass"):
            arrived(rows_of(0, x), x_recv.at[n, 0])
        block = rows_of(chunk_of(n), lax.rem(x - step_of(n) + NX, NX))
        remote(block, block, x_send, x_recv.at[n, 1], at(dx=step_of(n))).start()

    sign = 2 * core - 1

    def z_move(u, slot, hop, sem):
        remote(z_out.at[u, slot], z_in.at[u, slot], z_send, z_recv.at[u, sem], at(dz=hop * sign)).start()

    def z_wait(u, count, sem):
        with jax.named_scope(f"z_{sem}"):
            arrived(z_in.at[u, pl.ds(0, count)], z_recv.at[u, sem])

    def z_put(u, slot, offset, *added):
        value = prod[u, lax.rem(z + offset * sign + NZ, NZ)]
        for other in added:
            value = value + z_in[u, other].astype(jnp.float32)
        z_out[u, slot] = value.astype(jnp.bfloat16)

    def is_quick(u):
        return u >= CHUNKS - QUICK

    def first(u):
        if is_quick(u):
            moves = ((0, 4, 2, 0), (4, -3, -2, 0), (1, 3, 1, 0), (5, -2, -1, 0), (3, 1, 1, 3))
        else:
            moves = ((0, 4, 1, 0), (4, -3, -1, 0))
        for slot, offset, hop, sem in moves:
            z_put(u, slot, offset)
            z_move(u, slot, hop, sem)

    def mid(u, s):
        z_wait(u, 2 if s < 3 else 1, s - 1)
        z_put(u, s, 4 - s, s - 1)
        z_move(u, s, 1, s if s < 3 else 3)
        if s < 3:
            z_put(u, 4 + s, s - 3, 3 + s)
            z_move(u, 4 + s, -1, s if s < 2 else 3)

    def qmid(u):
        z_wait(u, 4, 0)
        z_put(u, 2, 2, 0, 1)
        z_move(u, 2, 2, 3)
        z_put(u, 6, -1, 4, 5)
        z_move(u, 6, -1, 3)

    def out_rows(chunk):
        return pl.ds(pl.multiple_of(chunk * MC, MC), MC)

    def last(u):
        added = (2, 3, 6) if is_quick(u) else (3, 6)
        z_wait(u, len(added), 3)
        value = prod[u, z]
        for other in added:
            value = value + z_in[u, other].astype(jnp.float32)
        value = value * (1.0 / (NZ * NX))
        n, second = UNITS[u]
        if second:
            o_out[n] = value.astype(jnp.bfloat16)
            remote(o_out.at[n], o_in.at[n], o_send, o_recv.at[n], at(dx=2)).start()
        else:
            out_ref[out_rows(chunk_of(n)), :] = value

    def o_last(n):
        with jax.named_scope("o"):
            arrived(o_in.at[0], o_recv.at[n])
        out_ref[out_rows(2 * n + 1 - half), :] = o_in[n].astype(jnp.float32)

    def product(u):
        n, second = UNITS[u]
        if not second:
            with jax.named_scope("x_last"):
                arrived(rows.at[0, pl.ds(0, 2 * tokens), :], x_recv.at[n, 1])
        turned[...] = rows[chunk_of(n)].T
        wide = 2 * NB

        def part(i, carry):
            at_i = pl.ds(pl.multiple_of(i * wide, wide), wide)
            value = jnp.dot(turned[...], cols[second, :, at_i], preferred_element_type=jnp.float32)
            prod[u, 2 * i] = value[:, :NB]
            prod[u, 2 * i + 1] = value[:, NB:]
            return carry

        with jax.named_scope("dot"):
            lax.fori_loop(0, NZ // 2, part, 0)
        first(u)

    def load(i):
        return (
            pltpu.make_async_copy(gate_hbm.at[:, lanes(i)], gate_buf.at[i], load_sem.at[i]),
            pltpu.make_async_copy(up_hbm.at[:, lanes(i)], up_buf.at[i], load_sem.at[i]),
        )

    def hide():
        def one(i, carry):
            for copy in load(i):
                copy.wait()
            gate = gate_buf[i].astype(jnp.float32)
            act = gate / (1.0 + jnp.exp(-gate))
            rows[i, row_block(x), :] = (act * up_buf[i].astype(jnp.float32)).astype(jnp.bfloat16)
            return carry

        for i in range(CHUNKS):
            for copy in load(i):
                copy.start()
        if PAIRS:
            cols[1, row_block(x), lanes(mine)] = grad_buf[lax.rem(x + 2, NX)]
        with jax.named_scope("hide"):
            lax.fori_loop(0, CHUNKS, one, 0)

    partners = (
        at(dz=1), at(dz=-1), at(dz=2), at(dz=-2), at(dx=1), at(dx=-1), at(dx=2), at(dy=1), at(dy=-1), at(dc=1),
    )
    barrier = pltpu.get_barrier_semaphore()
    for device in partners:
        pl.semaphore_signal(barrier, inc=1, device_id=device, device_id_type=MESH)
    grad_copy = [
        pltpu.make_async_copy(grad_hbm.at[:, pl.ds(k * NB, NB)], grad_buf.at[k], grad_sem) for k in range(NX)
    ]
    for copy in grad_copy:
        copy.start()
    with jax.named_scope("grad"):
        pltpu.make_async_copy(grad_buf, grad_buf, grad_sem).wait()
    cols[0, row_block(x), lanes(mine)] = grad_buf[x]
    with jax.named_scope("barrier"):
        pl.semaphore_wait(barrier, len(partners))

    steps = {
        "b_start": b_start, "b_own": b_own, "b_pass": b_pass, "b_far": b_far, "b_done": b_done, "hide": hide,
        "x_own": x_own, "x_pass": x_pass, "product": product, "mid": mid, "qmid": qmid, "last": last, "o_last": o_last,
    }
    for name, *arguments in ORDER:
        steps[name](*arguments)

    def sent(ref, sem):
        remote(ref, ref, sem, x_recv.at[0, 0], at(dx=1)).wait_send()

    with jax.named_scope("sent"):
        sent(rows.at[pl.ds(0, ITEMS), pl.ds(0, 3 * tokens), :], x_send)
        sets = 2 if PAIRS else 1
        sent(rows.at[pl.ds(0, sets), pl.ds(0, 3 * tokens), :], b_send.at[0])
        sent(rows.at[pl.ds(0, 3 * sets)], b_send.at[1])
        sent(rows.at[pl.ds(0, 4 * sets)], b_send.at[2])
        sent(z_out, z_send)
        if PAIRS:
            sent(o_out, o_send)


def solution(mesh):
    def shards(gate_pre, up_pre, out_grad):
        tokens, hidden = gate_pre.shape
        depth = NX * tokens
        dma = pltpu.SemaphoreType.DMA
        operands = [pltpu.with_memory_space_constraint(a, pltpu.HBM) for a in (gate_pre, up_pre, out_grad)]
        return pl.pallas_call(
            kernel,
            out_shape=jax.ShapeDtypeStruct((hidden, NB), jnp.float32),
            in_specs=[pl.BlockSpec(memory_space=pl.ANY)] * 3,
            out_specs=pl.BlockSpec(memory_space=pltpu.VMEM),
            scratch_shapes=[
                pltpu.VMEM((CHUNKS, tokens, MC), jnp.bfloat16),
                pltpu.VMEM((CHUNKS, tokens, MC), jnp.bfloat16),
                pltpu.VMEM((NX, tokens, NB), jnp.bfloat16),
                pltpu.VMEM((CHUNKS, depth, MC), jnp.bfloat16),
                pltpu.VMEM((MC, depth), jnp.bfloat16),
                pltpu.VMEM((2, depth, NZ * NB), jnp.bfloat16),
                pltpu.VMEM((CHUNKS, NZ, MC, NB), jnp.float32),
                pltpu.VMEM((CHUNKS, 7, MC, NB), jnp.bfloat16),
                pltpu.VMEM((CHUNKS, 7, MC, NB), jnp.bfloat16),
                pltpu.VMEM((max(PAIRS, 1), MC, NB), jnp.bfloat16),
                pltpu.VMEM((max(PAIRS, 1), MC, NB), jnp.bfloat16),
                dma((CHUNKS,)),
                dma,
                dma,
                dma((ITEMS, 2)),
                dma((3,)),
                dma((2, 3)),
                dma((2, NX, 2)),
                dma((2,)),
                dma,
                dma((CHUNKS, 4)),
                dma,
                dma((max(PAIRS, 1),)),
            ],
            compiler_params=pltpu.CompilerParams(
                collective_id=0, has_side_effects=True, vmem_limit_bytes=VMEM_BYTES
            ),
        )(*operands)

    return jax.shard_map(
        shards,
        mesh=mesh,
        in_specs=(P("node", "local"), P("node", "local"), P("node", "local")),
        out_specs=P("local", "node"),
        check_vma=False,
    )
```

```python
import jax
import jax.numpy as jnp
from jax import lax
from jax.experimental import pallas as pl
from jax.experimental.pallas import tpu as pltpu
from jax.sharding import PartitionSpec as P

MESH = pl.DeviceIdType.MESH
NZ, NX, NY, NC = 8, 4, 4, 2
MC = 128
NB = 128
CHUNKS = 15
PAIRS = 7
ITEMS = CHUNKS - PAIRS
UNITS = [(i, 0) for i in range(PAIRS)] + [(i, 1) for i in range(PAIRS)] + [(i, 0) for i in range(PAIRS, ITEMS)]
SPLIT = (0, 1, 7, 8)
QUICK = 0
VMEM_BYTES = 50_000_000
ORDER = (
    ("b_near", 0), ("b_own", 0, 0), ("hide",), ("b_far2", 0), ("b_own", 1, 0), ("b_near", 1), ("b_own", 0, 2),
    ("b_far2", 1), ("b_own", 0, 1), ("x_own", 0), ("x_own", 1), ("x_own", 2), ("b_own", 0, 3), ("b_own", 1, 1),
    ("b_own", 1, 2), ("x_pass", 0), ("b_own", 1, 3), ("b_take", 0, 1), ("b_pass", 0, 1), ("x_pass", 1),
    ("b_take", 0, 3), ("x_own", 3), ("b_take", 1, 1), ("b_take", 0, 0), ("b_pass", 0, 0), ("b_take", 0, 2),
    ("b_most", 0), ("b_take", 1, 0), ("x_pass", 2), ("b_pass", 0, 2), ("x_own", 4), ("b_pass", 0, 3),
    ("b_pass", 1, 1), ("part", 0, 0), ("b_pass", 1, 0), ("b_take", 1, 2), ("b_pass", 1, 2), ("x_pass", 3),
    ("b_take", 1, 3), ("b_pass", 1, 3), ("part", 1, 0), ("b_most", 1), ("part", 7, 0), ("b_far", 0, 1), ("x_pass", 4),
    ("b_far", 0, 2), ("x_own", 5), ("b_far", 0, 3), ("x_own", 6), ("b_far", 0, 0), ("part", 8, 0), ("pmid", 0, 1, 0),
    ("b_rest", 0), ("product", 2), ("b_far", 1, 0), ("part", 1, 1), ("pmid", 7, 1, 0), ("product", 3),
    ("b_far", 1, 1), ("pmid", 1, 1, 0), ("part", 0, 1), ("b_far", 1, 2), ("b_far", 1, 3), ("x_pass", 5),
    ("pmid", 8, 1, 0), ("product", 4), ("x_own", 7), ("mid", 2, 1), ("b_rest", 1), ("part", 8, 1), ("pmid", 7, 2, 0),
    ("product", 9), ("x_pass", 6), ("mid", 3, 1), ("product", 10), ("product", 11), ("mid", 4, 1), ("product", 5),
    ("product", 12), ("part", 7, 1), ("pmid", 0, 1, 1), ("mid", 9, 1), ("pmid", 8, 2, 0), ("mid", 10, 1),
    ("product", 6), ("x_pass", 7), ("product", 13), ("mid", 11, 1), ("mid", 12, 1), ("pmid", 7, 1, 1), ("mid", 5, 1),
    ("mid", 10, 2), ("mid", 2, 2), ("pmid", 8, 1, 1), ("pmid", 1, 2, 0), ("mid", 13, 1), ("product", 14),
    ("mid", 11, 2), ("pmid", 7, 2, 1), ("mid", 12, 2), ("mid", 9, 2), ("mid", 3, 2), ("mid", 10, 3),
    ("pmid", 8, 2, 1), ("mid", 13, 2), ("pmid", 1, 1, 1), ("pmid", 7, 3, 0), ("pmid", 0, 2, 1), ("mid", 14, 1),
    ("mid", 11, 3), ("mid", 6, 1), ("pmid", 8, 3, 0), ("mid", 12, 3), ("pmid", 7, 3, 1), ("mid", 9, 3),
    ("mid", 13, 3), ("mid", 4, 2), ("pmid", 8, 3, 1), ("last", 10), ("mid", 5, 2), ("mid", 14, 2), ("mid", 6, 2),
    ("pmid", 1, 2, 1), ("last", 11), ("pmid", 0, 2, 0), ("last", 12), ("plast", 7), ("mid", 2, 3), ("mid", 3, 3),
    ("last", 13), ("pmid", 1, 3, 0), ("last", 9), ("mid", 4, 3), ("pmid", 0, 3, 1), ("plast", 8), ("mid", 5, 3),
    ("mid", 14, 3), ("mid", 6, 3), ("pmid", 1, 3, 1), ("o_last", 3), ("pmid", 0, 3, 0), ("last", 2), ("o_last", 4),
    ("o_last", 5), ("o_last", 0), ("last", 5), ("last", 3), ("o_last", 6), ("last", 4), ("o_last", 1), ("o_last", 2),
    ("last", 14), ("plast", 1), ("last", 6), ("plast", 0),
)


def kernel(
    gate_hbm, up_hbm, grad_hbm, out_ref,
    gate_buf, up_buf, grad_buf, rows, turned, cols, prod, z_out, z_in, o_out, o_in,
    load_sem, grad_sem, x_send, x_recv, b_send, bx_recv, by_recv, bs_recv, z_send, z_recv, o_send, o_recv,
):
    tokens = grad_hbm.shape[0]
    node, local = lax.axis_index("node"), lax.axis_index("local")
    z, x = node // NX, node % NX
    y, core = local // NC, local % NC
    mine = y * NC + core

    def at(dz=0, dx=0, dy=0, dc=0):
        return {
            "node": lax.rem(z + dz + NZ, NZ) * NX + lax.rem(x + dx + NX, NX),
            "local": lax.rem(y + dy + NY, NY) * NC + lax.rem(core + dc, NC),
        }

    def remote(src, dst, send, recv, device):
        return pltpu.make_async_remote_copy(
            src_ref=src, dst_ref=dst, send_sem=send, recv_sem=recv, device_id=device, device_id_type=MESH
        )

    def arrived(ref, sem):
        remote(ref, ref, x_send, sem, at(dx=1)).wait_recv()

    def lanes(block):
        return pl.ds(pl.multiple_of(block * NB, NB), NB)

    def row_block(who):
        return pl.ds(pl.multiple_of(who * tokens, tokens), tokens)

    x_of = (x, lax.rem(x + NX - 1, NX), lax.rem(x + 1, NX), lax.rem(x + 2, NX))

    def piece(n, k, block):
        return cols.at[n, row_block(x_of[k]), lanes(block)]

    below = lax.rem(y + NY - 1, NY) * NC + core
    above = lax.rem(y + 1, NY) * NC + core
    across = lax.rem(y + 2, NY) * NC + core

    def b_send_to(n, k, dx):
        block = lax.rem(x + dx + 2 * n + NX, NX)
        remote(grad_buf.at[block], piece(n, 0, mine), b_send.at[0], bx_recv.at[n, k], at(dx=dx)).start()

    def b_near(n):
        b_send_to(n, 0, 1)
        b_send_to(n, 1, -1)

    def b_far2(n):
        b_send_to(n, 2, 2)

    def b_along(n, k, block, sem, dy):
        remote(piece(n, k, block), piece(n, k, block), b_send.at[1], sem, at(dy=dy)).start()

    def b_over(n, k, block, part=0):
        remote(piece(n, k, block), piece(n, k, block), b_send.at[2], bs_recv.at[n, part], at(dc=1)).start()

    def b_own(n, k):
        if k:
            with jax.named_scope(f"bx_{n}{k}"):
                arrived(grad_buf.at[0], bx_recv.at[n, k - 1])
        b_along(n, k, mine, by_recv.at[n, k, 0], 1)
        b_along(n, k, mine, by_recv.at[n, k, 0], -1)
        b_over(n, k, mine)

    def b_take(n, k):
        with jax.named_scope(f"by_{n}{k}"):
            arrived(rows.at[0, pl.ds(0, 2 * tokens), :], by_recv.at[n, k, 0])
        b_over(n, k, below)
        b_over(n, k, above)

    def b_pass(n, k):
        up = lax.rem(core + k, 2) == 0
        b_along(n, k, jnp.where(up, below, above), by_recv.at[n, k, 1], jnp.where(up, 1, -1))

    def b_far(n, k):
        with jax.named_scope(f"bf_{n}{k}"):
            arrived(grad_buf.at[0], by_recv.at[n, k, 1])
        b_over(n, k, across, 1)

    def b_most(n):
        with jax.named_scope(f"bm_{n}"):
            arrived(rows.at[pl.ds(0, 3)], bs_recv.at[n, 0])

    def b_rest(n):
        with jax.named_scope(f"br_{n}"):
            arrived(rows.at[0], bs_recv.at[n, 1])

    def rows_of(i, who):
        return rows.at[i, row_block(who), :]

    pair_step = 1 - 2 * lax.rem(x + core, 2)
    half = lax.rem(x - core + NX, NX) // 2

    def chunk_of(n):
        return 2 * n + half if n < PAIRS else n + PAIRS

    def step_of(n):
        return pair_step if n < PAIRS or n % 2 == 0 else -pair_step

    def x_own(n):
        mine_of, other = chunk_of(n), 2 * n + 1 - half if n < PAIRS else chunk_of(n)
        remote(rows_of(other, x), rows_of(other, x), x_send, x_recv.at[n, 0], at(dx=-step_of(n))).start()
        remote(rows_of(mine_of, x), rows_of(mine_of, x), x_send, x_recv.at[n, 1], at(dx=step_of(n))).start()

    def x_pass(n):
        with jax.named_scope("x_pass"):
            arrived(rows_of(0, x), x_recv.at[n, 0])
        block = rows_of(chunk_of(n), lax.rem(x - step_of(n) + NX, NX))
        remote(block, block, x_send, x_recv.at[n, 1], at(dx=step_of(n))).start()

    sign = 2 * core - 1

    def z_sem(u, sem):
        return z_recv.at[4 * u + 2 * sum(v < u for v in SPLIT) + sem]

    def z_move(u, slot, hop, sem):
        remote(z_out.at[u, slot], z_in.at[u, slot], z_send, z_sem(u, sem), at(dz=hop * sign)).start()

    def z_wait(u, count, sem):
        with jax.named_scope(f"z_{sem}"):
            arrived(z_in.at[u, pl.ds(0, count)], z_sem(u, sem))

    def block_at(offset):
        return lax.rem(z + offset * sign + NZ, NZ)

    def z_put(u, slot, offset, *added):
        value = prod[u, block_at(offset)]
        for other in added:
            value = value + z_in[u, other].astype(jnp.float32)
        z_out[u, slot] = value.astype(jnp.bfloat16)

    def is_quick(u):
        return u >= CHUNKS - QUICK

    def first(u):
        if is_quick(u):
            moves = ((0, 4, 2, 0), (4, -3, -2, 0), (1, 3, 1, 0), (5, -2, -1, 0), (3, 1, 1, 3))
        else:
            moves = ((0, 4, 1, 0), (4, -3, -1, 0))
        for slot, offset, hop, sem in moves:
            z_put(u, slot, offset)
            z_move(u, slot, hop, sem)

    def mid(u, s):
        z_wait(u, 2 if s < 3 else 1, s - 1)
        z_put(u, s, 4 - s, s - 1)
        z_move(u, s, 1, s if s < 3 else 3)
        if s < 3:
            z_put(u, 4 + s, s - 3, 3 + s)
            z_move(u, 4 + s, -1, s if s < 2 else 3)

    def qmid(u):
        z_wait(u, 4, 0)
        z_put(u, 2, 2, 0, 1)
        z_move(u, 2, 2, 3)
        z_put(u, 6, -1, 4, 5)
        z_move(u, 6, -1, 3)

    def if_part(offset, part, body):
        far = block_at(offset) // NC == lax.rem(y + 2, NY)
        pl.when(far if part else jnp.logical_not(far))(body)

    def pfirst(u, part):
        for slot, offset, hop, sem in ((0, 4, 1, 0), (4, -3, -1, 4)):
            def body(slot=slot, offset=offset, hop=hop, sem=sem):
                z_put(u, slot, offset)
                z_move(u, slot, hop, sem)
            if_part(offset, part, body)

    def pmid(u, s, part):
        def long():
            z_wait(u, 1, s - 1)
            z_put(u, s, 4 - s, s - 1)
            z_move(u, s, 1, s)

        def short():
            z_wait(u, 1, 3 + s)
            z_put(u, 4 + s, s - 3, 3 + s)
            z_move(u, 4 + s, -1, 4 + s if s < 2 else 3)

        if_part(4 - s, part, long)
        if s < 3:
            if_part(s - 3, part, short)

    def out_rows(chunk):
        return pl.ds(pl.multiple_of(chunk * MC, MC), MC)

    def last(u):
        added = (2, 3, 6) if is_quick(u) else (3, 6)
        z_wait(u, len(added), 3)
        value = prod[u, z]
        for other in added:
            value = value + z_in[u, other].astype(jnp.float32)
        value = value * (1.0 / (NZ * NX))
        n, second = UNITS[u]
        if second:
            o_out[n] = value.astype(jnp.bfloat16)
            remote(o_out.at[n], o_in.at[n], o_send, o_recv.at[n], at(dx=2)).start()
        else:
            out_ref[out_rows(chunk_of(n)), :] = value

    def o_last(n):
        with jax.named_scope("o"):
            arrived(o_in.at[0], o_recv.at[n])
        out_ref[out_rows(2 * n + 1 - half), :] = o_in[n].astype(jnp.float32)

    def rows_ready(u):
        n, second = UNITS[u]
        if not second:
            with jax.named_scope("x_last"):
                arrived(rows.at[0, pl.ds(0, 2 * tokens), :], x_recv.at[n, 1])
            turned[min(n, PAIRS)] = rows[chunk_of(n)].T

    def dot(u, place):
        n, second = UNITS[u]
        at_place = pl.ds(pl.multiple_of(place * NC * NB, NC * NB), NC * NB)
        value = jnp.dot(turned[min(n, PAIRS)], cols[second, :, at_place], preferred_element_type=jnp.float32)
        for i in range(NC):
            prod[u, NC * place + i] = value[:, i * NB : (i + 1) * NB]

    def product(u):
        rows_ready(u)
        with jax.named_scope("dot"):
            for place in range(NY):
                dot(u, place)
        first(u)

    def part(u, part):
        if part:
            dot(u, lax.rem(y + 2, NY))
        else:
            rows_ready(u)
            with jax.named_scope("dot"):
                for step in (0, 1, 3):
                    dot(u, lax.rem(y + step, NY))
        pfirst(u, part)

    def load(i):
        return (
            pltpu.make_async_copy(gate_hbm.at[:, lanes(i)], gate_buf.at[i], load_sem.at[i]),
            pltpu.make_async_copy(up_hbm.at[:, lanes(i)], up_buf.at[i], load_sem.at[i]),
        )

    def hide():
        def one(i, carry):
            for copy in load(i):
                copy.wait()
            gate = gate_buf[i].astype(jnp.float32)
            act = gate / (1.0 + jnp.exp(-gate))
            rows[i, row_block(x), :] = (act * up_buf[i].astype(jnp.float32)).astype(jnp.bfloat16)
            return carry

        for i in range(CHUNKS):
            for copy in load(i):
                copy.start()
        if PAIRS:
            cols[1, row_block(x), lanes(mine)] = grad_buf[lax.rem(x + 2, NX)]
        with jax.named_scope("hide"):
            lax.fori_loop(0, CHUNKS, one, 0)

    partners = (
        at(dz=1), at(dz=-1), at(dz=2), at(dz=-2), at(dx=1), at(dx=-1), at(dx=2), at(dy=1), at(dy=-1), at(dc=1),
    )
    barrier = pltpu.get_barrier_semaphore()
    for device in partners:
        pl.semaphore_signal(barrier, inc=1, device_id=device, device_id_type=MESH)
    grad_copy = [
        pltpu.make_async_copy(grad_hbm.at[:, pl.ds(k * NB, NB)], grad_buf.at[k], grad_sem) for k in range(NX)
    ]
    for copy in grad_copy:
        copy.start()
    with jax.named_scope("grad"):
        pltpu.make_async_copy(grad_buf, grad_buf, grad_sem).wait()
    cols[0, row_block(x), lanes(mine)] = grad_buf[x]
    with jax.named_scope("barrier"):
        pl.semaphore_wait(barrier, len(partners))

    steps = {
        "b_near": b_near, "b_far2": b_far2, "b_own": b_own, "b_take": b_take, "b_pass": b_pass, "b_far": b_far,
        "b_most": b_most, "b_rest": b_rest, "part": part, "pmid": pmid, "plast": last,
        "hide": hide, "x_own": x_own, "x_pass": x_pass, "product": product, "mid": mid, "qmid": qmid, "last": last,
        "o_last": o_last,
    }
    for name, *arguments in ORDER:
        steps[name](*arguments)

    def sent(ref, sem):
        remote(ref, ref, sem, x_recv.at[0, 0], at(dx=1)).wait_send()

    with jax.named_scope("sent"):
        sent(rows.at[pl.ds(0, ITEMS), pl.ds(0, 3 * tokens), :], x_send)
        sets = 2 if PAIRS else 1
        sent(rows.at[pl.ds(0, sets), pl.ds(0, 3 * tokens), :], b_send.at[0])
        sent(rows.at[pl.ds(0, 3 * sets)], b_send.at[1])
        sent(rows.at[pl.ds(0, 4 * sets)], b_send.at[2])
        sent(z_out, z_send)
        if PAIRS:
            sent(o_out, o_send)


def solution(mesh):
    def shards(gate_pre, up_pre, out_grad):
        tokens, hidden = gate_pre.shape
        depth = NX * tokens
        dma = pltpu.SemaphoreType.DMA
        operands = [pltpu.with_memory_space_constraint(a, pltpu.HBM) for a in (gate_pre, up_pre, out_grad)]
        return pl.pallas_call(
            kernel,
            out_shape=jax.ShapeDtypeStruct((hidden, NB), jnp.float32),
            in_specs=[pl.BlockSpec(memory_space=pl.ANY)] * 3,
            out_specs=pl.BlockSpec(memory_space=pltpu.VMEM),
            scratch_shapes=[
                pltpu.VMEM((CHUNKS, tokens, MC), jnp.bfloat16),
                pltpu.VMEM((CHUNKS, tokens, MC), jnp.bfloat16),
                pltpu.VMEM((NX, tokens, NB), jnp.bfloat16),
                pltpu.VMEM((CHUNKS, depth, MC), jnp.bfloat16),
                pltpu.VMEM((PAIRS + 1, MC, depth), jnp.bfloat16),
                pltpu.VMEM((2, depth, NZ * NB), jnp.bfloat16),
                pltpu.VMEM((CHUNKS, NZ, MC, NB), jnp.float32),
                pltpu.VMEM((CHUNKS, 7, MC, NB), jnp.bfloat16),
                pltpu.VMEM((CHUNKS, 7, MC, NB), jnp.bfloat16),
                pltpu.VMEM((max(PAIRS, 1), MC, NB), jnp.bfloat16),
                pltpu.VMEM((max(PAIRS, 1), MC, NB), jnp.bfloat16),
                dma((CHUNKS,)),
                dma,
                dma,
                dma((ITEMS, 2)),
                dma((3,)),
                dma((2, 3)),
                dma((2, NX, 2)),
                dma((2, 2)),
                dma,
                dma((4 * CHUNKS + 2 * len(SPLIT),)),
                dma,
                dma((max(PAIRS, 1),)),
            ],
            compiler_params=pltpu.CompilerParams(
                collective_id=0, has_side_effects=True, vmem_limit_bytes=VMEM_BYTES
            ),
        )(*operands)

    return jax.shard_map(
        shards,
        mesh=mesh,
        in_specs=(P("node", "local"), P("node", "local"), P("node", "local")),
        out_specs=P("local", "node"),
        check_vma=False,
    )
```

```python
import jax
import jax.numpy as jnp
from jax import lax
from jax.experimental import pallas as pl
from jax.experimental.pallas import tpu as pltpu
from jax.sharding import PartitionSpec as P

MESH = pl.DeviceIdType.MESH
NZ, NX, NY, NC = 8, 4, 4, 2
MC = 128
LOADS = 5
NB = 128
CHUNKS = 15
PAIRS = 6
ITEMS = CHUNKS - PAIRS
UNITS = [(i, 0) for i in range(PAIRS)] + [(i, 1) for i in range(PAIRS)] + [(i, 0) for i in range(PAIRS, ITEMS)]
SPLIT = (0, 1, 6)
QUICK = 0
VMEM_BYTES = 50_000_000
ORDER = (
    ("b_near", 0), ("b_own", 0, 0), ("hide",), ("b_own", 1, 0), ("b_far2", 0), ("x_own", 0), ("x_own", 1),
    ("b_own", 0, 1), ("b_own", 0, 2), ("b_near", 1), ("b_take", 1, 0), ("x_pass", 0), ("b_far2", 1), ("b_own", 0, 3),
    ("b_take", 0, 1), ("x_pass", 1), ("b_pass", 0, 1), ("b_take", 0, 2), ("b_pass", 0, 2), ("x_own", 2),
    ("b_own", 1, 2), ("b_take", 0, 3), ("b_take", 0, 0), ("b_most", 0), ("b_own", 1, 1), ("b_pass", 0, 3),
    ("b_pass", 0, 0), ("x_own", 3), ("part", 0, 0), ("b_far", 0, 1), ("b_far", 0, 2), ("b_take", 1, 2), ("x_pass", 2),
    ("x_own", 4), ("b_own", 1, 3), ("part", 1, 0), ("b_take", 1, 1), ("pmid", 0, 1, 0), ("b_pass", 1, 2),
    ("b_far", 0, 0), ("b_pass", 1, 1), ("b_far", 0, 3), ("b_pass", 1, 0), ("x_pass", 3), ("x_pass", 4), ("b_rest", 0),
    ("part", 1, 1), ("part", 0, 1), ("pmid", 1, 1, 0), ("b_take", 1, 3), ("b_pass", 1, 3), ("x_own", 5),
    ("pmid", 0, 2, 0), ("product", 2), ("b_most", 1), ("part", 6, 0), ("x_own", 6), ("product", 3), ("pmid", 1, 1, 1),
    ("b_far", 1, 2), ("pmid", 0, 1, 1), ("pmid", 1, 2, 0), ("b_far", 1, 1), ("b_far", 1, 0), ("product", 4),
    ("b_far", 1, 3), ("pmid", 0, 3, 0), ("mid", 2, 1), ("x_pass", 5), ("x_own", 7), ("x_own", 8), ("pmid", 6, 1, 0),
    ("b_rest", 1), ("product", 8), ("x_pass", 6), ("mid", 3, 1), ("product", 7), ("part", 6, 1), ("mid", 4, 1),
    ("product", 10), ("pmid", 1, 2, 1), ("product", 9), ("mid", 8, 1), ("product", 5), ("x_pass", 7), ("x_pass", 8),
    ("pmid", 6, 1, 1), ("mid", 2, 2), ("product", 11), ("mid", 10, 1), ("pmid", 0, 2, 1), ("pmid", 6, 2, 0),
    ("mid", 9, 1), ("mid", 7, 1), ("mid", 5, 1), ("product", 12), ("mid", 11, 1), ("mid", 8, 2), ("product", 14),
    ("product", 13), ("pmid", 6, 2, 1), ("mid", 7, 2), ("mid", 10, 2), ("mid", 9, 2), ("mid", 12, 1), ("mid", 11, 2),
    ("mid", 3, 2), ("mid", 14, 1), ("pmid", 6, 3, 1), ("mid", 13, 1), ("mid", 7, 3), ("mid", 9, 3), ("mid", 5, 2),
    ("mid", 8, 3), ("pmid", 6, 3, 0), ("mid", 11, 3), ("mid", 10, 3), ("mid", 4, 2), ("mid", 14, 2), ("mid", 12, 2),
    ("mid", 13, 2), ("pmid", 0, 3, 1), ("mid", 3, 3), ("pmid", 1, 3, 0), ("last", 7), ("last", 9), ("last", 8),
    ("plast", 6), ("pmid", 1, 3, 1), ("mid", 5, 3), ("last", 11), ("mid", 2, 3), ("last", 10), ("mid", 4, 3),
    ("mid", 14, 3), ("mid", 12, 3), ("mid", 13, 3), ("last", 5), ("last", 2), ("o_last", 1), ("last", 4),
    ("plast", 1), ("o_last", 0), ("last", 3), ("o_last", 5), ("o_last", 2), ("last", 14), ("plast", 0), ("o_last", 3),
    ("last", 12), ("o_last", 4), ("last", 13),
)


def kernel(
    gate_hbm, up_hbm, grad_hbm, out_ref,
    gate_buf, up_buf, grad_buf, rows, turned, cols, prod, z_out, z_in, o_out, o_in,
    load_sem, grad_sem, x_send, x_recv, b_send, bx_recv, by_recv, bs_recv, z_send, z_recv, o_send, o_recv,
):
    tokens = grad_hbm.shape[0]
    node, local = lax.axis_index("node"), lax.axis_index("local")
    z, x = node // NX, node % NX
    y, core = local // NC, local % NC
    mine = y * NC + core

    def at(dz=0, dx=0, dy=0, dc=0):
        return {
            "node": lax.rem(z + dz + NZ, NZ) * NX + lax.rem(x + dx + NX, NX),
            "local": lax.rem(y + dy + NY, NY) * NC + lax.rem(core + dc, NC),
        }

    def remote(src, dst, send, recv, device):
        return pltpu.make_async_remote_copy(
            src_ref=src, dst_ref=dst, send_sem=send, recv_sem=recv, device_id=device, device_id_type=MESH
        )

    def arrived(ref, sem):
        remote(ref, ref, x_send, sem, at(dx=1)).wait_recv()

    def lanes(block):
        return pl.ds(pl.multiple_of(block * NB, NB), NB)

    def row_block(who):
        return pl.ds(pl.multiple_of(who * tokens, tokens), tokens)

    x_of = (x, lax.rem(x + NX - 1, NX), lax.rem(x + 1, NX), lax.rem(x + 2, NX))

    def piece(n, k, block):
        return cols.at[n, row_block(x_of[k]), lanes(block)]

    below = lax.rem(y + NY - 1, NY) * NC + core
    above = lax.rem(y + 1, NY) * NC + core
    across = lax.rem(y + 2, NY) * NC + core

    def b_send_to(n, k, dx):
        block = lax.rem(x + dx + 2 * n + NX, NX)
        remote(grad_buf.at[block], piece(n, 0, mine), b_send.at[0], bx_recv.at[n, k], at(dx=dx)).start()

    def b_near(n):
        b_send_to(n, 0, 1)
        b_send_to(n, 1, -1)

    def b_far2(n):
        b_send_to(n, 2, 2)

    def b_along(n, k, block, sem, dy):
        remote(piece(n, k, block), piece(n, k, block), b_send.at[1], sem, at(dy=dy)).start()

    def b_over(n, k, block, part=0):
        remote(piece(n, k, block), piece(n, k, block), b_send.at[2], bs_recv.at[n, part], at(dc=1)).start()

    def b_own(n, k):
        if k:
            with jax.named_scope(f"bx_{n}{k}"):
                arrived(grad_buf.at[0], bx_recv.at[n, k - 1])
        b_along(n, k, mine, by_recv.at[n, k, 0], 1)
        b_along(n, k, mine, by_recv.at[n, k, 0], -1)
        b_over(n, k, mine)

    def b_take(n, k):
        with jax.named_scope(f"by_{n}{k}"):
            arrived(rows.at[0, pl.ds(0, 2 * tokens), :], by_recv.at[n, k, 0])
        b_over(n, k, below)
        b_over(n, k, above)

    def b_pass(n, k):
        up = lax.rem(core + k, 2) == 0
        b_along(n, k, jnp.where(up, below, above), by_recv.at[n, k, 1], jnp.where(up, 1, -1))

    def b_far(n, k):
        with jax.named_scope(f"bf_{n}{k}"):
            arrived(grad_buf.at[0], by_recv.at[n, k, 1])
        b_over(n, k, across, 1)

    def b_most(n):
        with jax.named_scope(f"bm_{n}"):
            arrived(rows.at[pl.ds(0, 3)], bs_recv.at[n, 0])

    def b_rest(n):
        with jax.named_scope(f"br_{n}"):
            arrived(rows.at[0], bs_recv.at[n, 1])

    def rows_of(i, who):
        return rows.at[i, row_block(who), :]

    pair_step = 1 - 2 * lax.rem(x + core, 2)
    half = lax.rem(x - core + NX, NX) // 2

    def chunk_of(n):
        return 2 * n + half if n < PAIRS else n + PAIRS

    def step_of(n):
        return pair_step if n < PAIRS or n % 2 == 0 else -pair_step

    def x_own(n):
        mine_of, other = chunk_of(n), 2 * n + 1 - half if n < PAIRS else chunk_of(n)
        remote(rows_of(other, x), rows_of(other, x), x_send, x_recv.at[n, 0], at(dx=-step_of(n))).start()
        remote(rows_of(mine_of, x), rows_of(mine_of, x), x_send, x_recv.at[n, 1], at(dx=step_of(n))).start()

    def x_pass(n):
        with jax.named_scope("x_pass"):
            arrived(rows_of(0, x), x_recv.at[n, 0])
        block = rows_of(chunk_of(n), lax.rem(x - step_of(n) + NX, NX))
        remote(block, block, x_send, x_recv.at[n, 1], at(dx=step_of(n))).start()

    sign = 2 * core - 1

    def z_sem(u, sem):
        return z_recv.at[4 * u + 2 * sum(v < u for v in SPLIT) + sem]

    def z_move(u, slot, hop, sem):
        remote(z_out.at[u, slot], z_in.at[u, slot], z_send, z_sem(u, sem), at(dz=hop * sign)).start()

    def z_wait(u, count, sem):
        with jax.named_scope(f"z_{sem}"):
            arrived(z_in.at[u, pl.ds(0, count)], z_sem(u, sem))

    def block_at(offset):
        return lax.rem(z + offset * sign + NZ, NZ)

    def z_put(u, slot, offset, *added):
        value = prod[u, block_at(offset)]
        for other in added:
            value = value + z_in[u, other].astype(jnp.float32)
        z_out[u, slot] = value.astype(jnp.bfloat16)

    def is_quick(u):
        return u >= CHUNKS - QUICK

    def first(u):
        if is_quick(u):
            moves = ((0, 4, 2, 0), (4, -3, -2, 0), (1, 3, 1, 0), (5, -2, -1, 0), (3, 1, 1, 3))
        else:
            moves = ((0, 4, 1, 0), (4, -3, -1, 0))
        for slot, offset, hop, sem in moves:
            z_put(u, slot, offset)
            z_move(u, slot, hop, sem)

    def mid(u, s):
        z_wait(u, 2 if s < 3 else 1, s - 1)
        z_put(u, s, 4 - s, s - 1)
        z_move(u, s, 1, s if s < 3 else 3)
        if s < 3:
            z_put(u, 4 + s, s - 3, 3 + s)
            z_move(u, 4 + s, -1, s if s < 2 else 3)

    def qmid(u):
        z_wait(u, 4, 0)
        z_put(u, 2, 2, 0, 1)
        z_move(u, 2, 2, 3)
        z_put(u, 6, -1, 4, 5)
        z_move(u, 6, -1, 3)

    def if_part(offset, part, body):
        far = block_at(offset) // NC == lax.rem(y + 2, NY)
        pl.when(far if part else jnp.logical_not(far))(body)

    def pfirst(u, part):
        for slot, offset, hop, sem in ((0, 4, 1, 0), (4, -3, -1, 4)):
            def body(slot=slot, offset=offset, hop=hop, sem=sem):
                z_put(u, slot, offset)
                z_move(u, slot, hop, sem)
            if_part(offset, part, body)

    def pmid(u, s, part):
        def long():
            z_wait(u, 1, s - 1)
            z_put(u, s, 4 - s, s - 1)
            z_move(u, s, 1, s)

        def short():
            z_wait(u, 1, 3 + s)
            z_put(u, 4 + s, s - 3, 3 + s)
            z_move(u, 4 + s, -1, 4 + s if s < 2 else 3)

        if_part(4 - s, part, long)
        if s < 3:
            if_part(s - 3, part, short)

    def out_rows(chunk):
        return pl.ds(pl.multiple_of(chunk * MC, MC), MC)

    def last(u):
        added = (2, 3, 6) if is_quick(u) else (3, 6)
        z_wait(u, len(added), 3)
        value = prod[u, z]
        for other in added:
            value = value + z_in[u, other].astype(jnp.float32)
        value = value * (1.0 / (NZ * NX))
        n, second = UNITS[u]
        if second:
            o_out[n] = value.astype(jnp.bfloat16)
            remote(o_out.at[n], o_in.at[n], o_send, o_recv.at[n], at(dx=2)).start()
        else:
            out_ref[out_rows(chunk_of(n)), :] = value

    def o_last(n):
        with jax.named_scope("o"):
            arrived(o_in.at[0], o_recv.at[n])
        out_ref[out_rows(2 * n + 1 - half), :] = o_in[n].astype(jnp.float32)

    def rows_ready(u):
        n, second = UNITS[u]
        if not second:
            with jax.named_scope("x_last"):
                arrived(rows.at[0, pl.ds(0, 2 * tokens), :], x_recv.at[n, 1])
            turned[min(n, PAIRS)] = rows[chunk_of(n)].T

    def dot(u, place):
        n, second = UNITS[u]
        at_place = pl.ds(pl.multiple_of(place * NC * NB, NC * NB), NC * NB)
        value = jnp.dot(turned[min(n, PAIRS)], cols[second, :, at_place], preferred_element_type=jnp.float32)
        for i in range(NC):
            prod[u, NC * place + i] = value[:, i * NB : (i + 1) * NB]

    def product(u):
        rows_ready(u)
        with jax.named_scope("dot"):
            for place in range(NY):
                dot(u, place)
        first(u)

    def part(u, part):
        if part:
            dot(u, lax.rem(y + 2, NY))
        else:
            rows_ready(u)
            with jax.named_scope("dot"):
                for step in (0, 1, 3):
                    dot(u, lax.rem(y + step, NY))
        pfirst(u, part)

    def load(i):
        return (
            pltpu.make_async_copy(gate_hbm.at[:, lanes(i)], gate_buf.at[i], load_sem.at[i // LOADS]),
            pltpu.make_async_copy(up_hbm.at[:, lanes(i)], up_buf.at[i], load_sem.at[i // LOADS]),
        )

    def hide():
        def one(i, carry):
            gate = gate_buf[i].astype(jnp.float32)
            act = gate / (1.0 + jnp.exp(-gate))
            rows[i, row_block(x), :] = (act * up_buf[i].astype(jnp.float32)).astype(jnp.bfloat16)
            return carry

        for i in range(CHUNKS):
            for copy in load(i):
                copy.start()
        if PAIRS:
            cols[1, row_block(x), lanes(mine)] = grad_buf[lax.rem(x + 2, NX)]
        with jax.named_scope("hide"):
            for group in range(CHUNKS // LOADS):
                both = gate_buf.at[pl.ds(0, 2 * LOADS)]
                pltpu.make_async_copy(both, both, load_sem.at[group]).wait()
                lax.fori_loop(group * LOADS, (group + 1) * LOADS, one, 0)

    partners = (
        at(dz=1), at(dz=-1), at(dz=2), at(dz=-2), at(dx=1), at(dx=-1), at(dx=2), at(dy=1), at(dy=-1), at(dc=1),
    )
    barrier = pltpu.get_barrier_semaphore()
    for device in partners:
        pl.semaphore_signal(barrier, inc=1, device_id=device, device_id_type=MESH)
    grad_copy = [
        pltpu.make_async_copy(grad_hbm.at[:, pl.ds(k * NB, NB)], grad_buf.at[k], grad_sem) for k in range(NX)
    ]
    for copy in grad_copy:
        copy.start()
    with jax.named_scope("grad"):
        pltpu.make_async_copy(grad_buf, grad_buf, grad_sem).wait()
    cols[0, row_block(x), lanes(mine)] = grad_buf[x]
    with jax.named_scope("barrier"):
        pl.semaphore_wait(barrier, len(partners))

    steps = {
        "b_near": b_near, "b_far2": b_far2, "b_own": b_own, "b_take": b_take, "b_pass": b_pass, "b_far": b_far,
        "b_most": b_most, "b_rest": b_rest, "part": part, "pmid": pmid, "plast": last,
        "hide": hide, "x_own": x_own, "x_pass": x_pass, "product": product, "mid": mid, "qmid": qmid, "last": last,
        "o_last": o_last,
    }
    for name, *arguments in ORDER:
        steps[name](*arguments)

    def sent(ref, sem):
        remote(ref, ref, sem, x_recv.at[0, 0], at(dx=1)).wait_send()

    with jax.named_scope("sent"):
        sent(rows.at[pl.ds(0, ITEMS), pl.ds(0, 3 * tokens), :], x_send)
        sets = 2 if PAIRS else 1
        sent(rows.at[pl.ds(0, sets), pl.ds(0, 3 * tokens), :], b_send.at[0])
        sent(rows.at[pl.ds(0, 3 * sets)], b_send.at[1])
        sent(rows.at[pl.ds(0, 4 * sets)], b_send.at[2])
        sent(z_out, z_send)
        if PAIRS:
            sent(o_out, o_send)


def solution(mesh):
    def shards(gate_pre, up_pre, out_grad):
        tokens, hidden = gate_pre.shape
        depth = NX * tokens
        dma = pltpu.SemaphoreType.DMA
        operands = [pltpu.with_memory_space_constraint(a, pltpu.HBM) for a in (gate_pre, up_pre, out_grad)]
        return pl.pallas_call(
            kernel,
            out_shape=jax.ShapeDtypeStruct((hidden, NB), jnp.float32),
            in_specs=[pl.BlockSpec(memory_space=pl.ANY)] * 3,
            out_specs=pl.BlockSpec(memory_space=pltpu.VMEM),
            scratch_shapes=[
                pltpu.VMEM((CHUNKS, tokens, MC), jnp.bfloat16),
                pltpu.VMEM((CHUNKS, tokens, MC), jnp.bfloat16),
                pltpu.VMEM((NX, tokens, NB), jnp.bfloat16),
                pltpu.VMEM((CHUNKS, depth, MC), jnp.bfloat16),
                pltpu.VMEM((PAIRS + 1, MC, depth), jnp.bfloat16),
                pltpu.VMEM((2, depth, NZ * NB), jnp.bfloat16),
                pltpu.VMEM((CHUNKS, NZ, MC, NB), jnp.float32),
                pltpu.VMEM((CHUNKS, 7, MC, NB), jnp.bfloat16),
                pltpu.VMEM((CHUNKS, 7, MC, NB), jnp.bfloat16),
                pltpu.VMEM((max(PAIRS, 1), MC, NB), jnp.bfloat16),
                pltpu.VMEM((max(PAIRS, 1), MC, NB), jnp.bfloat16),
                dma((CHUNKS // LOADS,)),
                dma,
                dma,
                dma((ITEMS, 2)),
                dma((3,)),
                dma((2, 3)),
                dma((2, NX, 2)),
                dma((2, 2)),
                dma,
                dma((4 * CHUNKS + 2 * len(SPLIT),)),
                dma,
                dma((max(PAIRS, 1),)),
            ],
            compiler_params=pltpu.CompilerParams(
                collective_id=0, has_side_effects=True, vmem_limit_bytes=VMEM_BYTES
            ),
        )(*operands)

    return jax.shard_map(
        shards,
        mesh=mesh,
        in_specs=(P("node", "local"), P("node", "local"), P("node", "local")),
        out_specs=P("local", "node"),
        check_vma=False,
    )
```

```python
import jax
import jax.numpy as jnp
from jax import lax
from jax.experimental import pallas as pl
from jax.experimental.pallas import tpu as pltpu
from jax.sharding import PartitionSpec as P

MESH = pl.DeviceIdType.MESH
NZ, NX, NY, NC = 8, 4, 4, 2
MC = 128
LOADS = 5
NB = 128
CHUNKS = 15
PAIRS = 6
ITEMS = CHUNKS - PAIRS
UNITS = [(i, 0) for i in range(PAIRS)] + [(i, 1) for i in range(PAIRS)] + [(i, 0) for i in range(PAIRS, ITEMS)]
SPLIT = (0, 1, 6)
QUICK = 0
VMEM_BYTES = 50_000_000
ORDER = (
    ("b_near", 0), ("b_own", 0, 0), ("hide",), ("b_own", 1, 0), ("b_far2", 0), ("x_own", 0), ("x_own", 1),
    ("b_own", 0, 1), ("b_own", 0, 2), ("b_near", 1), ("b_take", 1, 0), ("x_pass", 0), ("b_far2", 1), ("b_own", 0, 3),
    ("b_take", 0, 1), ("x_pass", 1), ("b_pass", 0, 1), ("b_take", 0, 2), ("b_pass", 0, 2), ("x_own", 2),
    ("b_own", 1, 2), ("b_take", 0, 3), ("b_take", 0, 0), ("b_most", 0), ("b_own", 1, 1), ("b_pass", 0, 3),
    ("b_pass", 0, 0), ("x_own", 3), ("part", 0, 0), ("b_far", 0, 1), ("b_far", 0, 2), ("b_take", 1, 2), ("x_pass", 2),
    ("x_own", 4), ("b_own", 1, 3), ("part", 1, 0), ("b_take", 1, 1), ("x_pass", 3), ("pmid", 0, 1, 0),
    ("b_pass", 1, 2), ("b_far", 0, 0), ("b_pass", 1, 1), ("b_far", 0, 3), ("b_pass", 1, 0), ("x_pass", 4),
    ("b_rest", 0), ("part", 1, 1), ("part", 0, 1), ("pmid", 1, 1, 0), ("b_take", 1, 3), ("x_own", 5),
    ("b_pass", 1, 3), ("pmid", 0, 2, 0), ("product", 2), ("b_most", 1), ("part", 6, 0), ("x_own", 6), ("product", 3),
    ("pmid", 1, 1, 1), ("b_far", 1, 2), ("pmid", 0, 1, 1), ("product", 4), ("pmid", 1, 2, 0), ("b_far", 1, 1),
    ("b_far", 1, 0), ("b_far", 1, 3), ("mid", 2, 1), ("x_pass", 5), ("x_own", 7), ("x_own", 8), ("pmid", 0, 3, 0),
    ("pmid", 6, 1, 0), ("b_rest", 1), ("part", 6, 1), ("product", 8), ("x_pass", 6), ("mid", 3, 1), ("product", 7),
    ("mid", 4, 1), ("product", 10), ("pmid", 1, 2, 1), ("product", 9), ("mid", 8, 1), ("product", 5), ("x_pass", 7),
    ("x_pass", 8), ("pmid", 6, 1, 1), ("mid", 2, 2), ("product", 11), ("mid", 10, 1), ("pmid", 0, 2, 1),
    ("pmid", 6, 2, 0), ("mid", 9, 1), ("mid", 7, 1), ("mid", 5, 1), ("product", 12), ("mid", 11, 1), ("mid", 8, 2),
    ("product", 14), ("product", 13), ("pmid", 6, 2, 1), ("mid", 7, 2), ("mid", 10, 2), ("mid", 9, 2), ("mid", 12, 1),
    ("mid", 11, 2), ("mid", 3, 2), ("mid", 14, 1), ("pmid", 6, 3, 1), ("mid", 13, 1), ("mid", 7, 3), ("mid", 9, 3),
    ("mid", 5, 2), ("mid", 8, 3), ("pmid", 6, 3, 0), ("mid", 11, 3), ("mid", 10, 3), ("mid", 4, 2), ("mid", 14, 2),
    ("mid", 12, 2), ("mid", 13, 2), ("pmid", 0, 3, 1), ("mid", 3, 3), ("pmid", 1, 3, 0), ("last", 7), ("last", 9),
    ("last", 8), ("plast", 6), ("pmid", 1, 3, 1), ("mid", 5, 3), ("last", 11), ("mid", 2, 3), ("last", 10),
    ("mid", 4, 3), ("mid", 14, 3), ("mid", 12, 3), ("mid", 13, 3), ("last", 5), ("last", 4), ("last", 2),
    ("o_last", 1), ("plast", 1), ("o_last", 0), ("last", 3), ("o_last", 5), ("o_last", 2), ("last", 14),
    ("o_last", 3), ("last", 12), ("o_last", 4), ("plast", 0), ("last", 13),
)


def kernel(
    gate_hbm, up_hbm, grad_hbm, out_ref,
    gate_buf, up_buf, grad_buf, rows, turned, cols, prod, z_out, z_in, o_out, o_in,
    load_sem, grad_sem, x_send, x_recv, b_send, bx_recv, by_recv, bs_recv, z_send, z_recv, o_send, o_recv,
):
    tokens = grad_hbm.shape[0]
    node, local = lax.axis_index("node"), lax.axis_index("local")
    z, x = node // NX, node % NX
    y, core = local // NC, local % NC
    mine = y * NC + core

    def at(dz=0, dx=0, dy=0, dc=0):
        return {
            "node": lax.rem(z + dz + NZ, NZ) * NX + lax.rem(x + dx + NX, NX),
            "local": lax.rem(y + dy + NY, NY) * NC + lax.rem(core + dc, NC),
        }

    def remote(src, dst, send, recv, device):
        return pltpu.make_async_remote_copy(
            src_ref=src, dst_ref=dst, send_sem=send, recv_sem=recv, device_id=device, device_id_type=MESH
        )

    def arrived(ref, sem):
        remote(ref, ref, x_send, sem, at(dx=1)).wait_recv()

    def lanes(block):
        return pl.ds(pl.multiple_of(block * NB, NB), NB)

    def row_block(who):
        return pl.ds(pl.multiple_of(who * tokens, tokens), tokens)

    x_of = (x, lax.rem(x + NX - 1, NX), lax.rem(x + 1, NX), lax.rem(x + 2, NX))

    def piece(n, k, block):
        return cols.at[n, row_block(x_of[k]), lanes(block)]

    below = lax.rem(y + NY - 1, NY) * NC + core
    above = lax.rem(y + 1, NY) * NC + core
    across = lax.rem(y + 2, NY) * NC + core

    def b_send_to(n, k, dx):
        block = lax.rem(x + dx + 2 * n + NX, NX)
        remote(grad_buf.at[block], piece(n, 0, mine), b_send.at[0], bx_recv.at[n, k], at(dx=dx)).start()

    def b_near(n):
        b_send_to(n, 0, 1)
        b_send_to(n, 1, -1)

    def b_far2(n):
        b_send_to(n, 2, 2)

    def b_along(n, k, block, sem, dy):
        remote(piece(n, k, block), piece(n, k, block), b_send.at[1], sem, at(dy=dy)).start()

    def b_over(n, k, block, part=0):
        remote(piece(n, k, block), piece(n, k, block), b_send.at[2], bs_recv.at[n, part], at(dc=1)).start()

    def b_own(n, k):
        if k:
            with jax.named_scope(f"bx_{n}{k}"):
                arrived(grad_buf.at[0], bx_recv.at[n, k - 1])
        b_along(n, k, mine, by_recv.at[n, k, 0], 1)
        b_along(n, k, mine, by_recv.at[n, k, 0], -1)
        b_over(n, k, mine)

    def b_take(n, k):
        with jax.named_scope(f"by_{n}{k}"):
            arrived(rows.at[0, pl.ds(0, 2 * tokens), :], by_recv.at[n, k, 0])
        b_over(n, k, below)
        b_over(n, k, above)

    def b_pass(n, k):
        up = lax.rem(core + k, 2) == 0
        b_along(n, k, jnp.where(up, below, above), by_recv.at[n, k, 1], jnp.where(up, 1, -1))

    def b_far(n, k):
        with jax.named_scope(f"bf_{n}{k}"):
            arrived(grad_buf.at[0], by_recv.at[n, k, 1])
        b_over(n, k, across, 1)

    def b_most(n):
        with jax.named_scope(f"bm_{n}"):
            arrived(rows.at[pl.ds(0, 3)], bs_recv.at[n, 0])

    def b_rest(n):
        with jax.named_scope(f"br_{n}"):
            arrived(rows.at[0], bs_recv.at[n, 1])

    def rows_of(i, who):
        return rows.at[i, row_block(who), :]

    pair_step = 1 - 2 * lax.rem(x + core, 2)
    half = lax.rem(x - core + NX, NX) // 2

    def chunk_of(n):
        return 2 * n + half if n < PAIRS else n + PAIRS

    def step_of(n):
        return pair_step if n < PAIRS or n % 2 == 0 else -pair_step

    def x_own(n):
        mine_of, other = chunk_of(n), 2 * n + 1 - half if n < PAIRS else chunk_of(n)
        remote(rows_of(other, x), rows_of(other, x), x_send, x_recv.at[n, 0], at(dx=-step_of(n))).start()
        remote(rows_of(mine_of, x), rows_of(mine_of, x), x_send, x_recv.at[n, 1], at(dx=step_of(n))).start()

    def x_pass(n):
        with jax.named_scope("x_pass"):
            arrived(rows_of(0, x), x_recv.at[n, 0])
        block = rows_of(chunk_of(n), lax.rem(x - step_of(n) + NX, NX))
        remote(block, block, x_send, x_recv.at[n, 1], at(dx=step_of(n))).start()

    sign = 2 * core - 1

    def z_sem(u, sem):
        return z_recv.at[4 * u + 2 * sum(v < u for v in SPLIT) + sem]

    def z_move(u, slot, hop, sem):
        remote(z_out.at[u, slot], z_in.at[u, slot], z_send, z_sem(u, sem), at(dz=hop * sign)).start()

    def z_wait(u, count, sem):
        with jax.named_scope(f"z_{sem}"):
            arrived(z_in.at[u, pl.ds(0, count)], z_sem(u, sem))

    def block_at(offset):
        return lax.rem(z + offset * sign + NZ, NZ)

    def z_put(u, slot, offset, *added):
        value = prod[u, block_at(offset)]
        for other in added:
            value = value + z_in[u, other].astype(jnp.float32)
        z_out[u, slot] = value.astype(jnp.bfloat16)

    def is_quick(u):
        return u >= CHUNKS - QUICK

    def first(u):
        if is_quick(u):
            moves = ((0, 4, 2, 0), (4, -3, -2, 0), (1, 3, 1, 0), (5, -2, -1, 0), (3, 1, 1, 3))
        else:
            moves = ((0, 4, 1, 0), (4, -3, -1, 0))
        for slot, offset, hop, sem in moves:
            z_put(u, slot, offset)
            z_move(u, slot, hop, sem)

    def mid(u, s):
        z_wait(u, 2 if s < 3 else 1, s - 1)
        z_put(u, s, 4 - s, s - 1)
        z_move(u, s, 1, s if s < 3 else 3)
        if s < 3:
            z_put(u, 4 + s, s - 3, 3 + s)
            z_move(u, 4 + s, -1, s if s < 2 else 3)

    def qmid(u):
        z_wait(u, 4, 0)
        z_put(u, 2, 2, 0, 1)
        z_move(u, 2, 2, 3)
        z_put(u, 6, -1, 4, 5)
        z_move(u, 6, -1, 3)

    def if_part(offset, part, body):
        far = block_at(offset) // NC == lax.rem(y + 2, NY)
        pl.when(far if part else jnp.logical_not(far))(body)

    def pfirst(u, part):
        for slot, offset, hop, sem in ((0, 4, 1, 0), (4, -3, -1, 4)):
            def body(slot=slot, offset=offset, hop=hop, sem=sem):
                z_put(u, slot, offset)
                z_move(u, slot, hop, sem)
            if_part(offset, part, body)

    def pmid(u, s, part):
        def long():
            z_wait(u, 1, s - 1)
            z_put(u, s, 4 - s, s - 1)
            z_move(u, s, 1, s)

        def short():
            z_wait(u, 1, 3 + s)
            z_put(u, 4 + s, s - 3, 3 + s)
            z_move(u, 4 + s, -1, 4 + s if s < 2 else 3)

        if_part(4 - s, part, long)
        if s < 3:
            if_part(s - 3, part, short)

    def out_rows(chunk):
        return pl.ds(pl.multiple_of(chunk * MC, MC), MC)

    def last(u):
        added = (2, 3, 6) if is_quick(u) else (3, 6)
        z_wait(u, len(added), 3)
        value = prod[u, z]
        for other in added:
            value = value + z_in[u, other].astype(jnp.float32)
        value = value * (1.0 / (NZ * NX))
        n, second = UNITS[u]
        if second:
            o_out[n] = value.astype(jnp.bfloat16)
            remote(o_out.at[n], o_in.at[n], o_send, o_recv.at[n], at(dx=2)).start()
        else:
            out_ref[out_rows(chunk_of(n)), :] = value

    def o_last(n):
        with jax.named_scope("o"):
            arrived(o_in.at[0], o_recv.at[n])
        out_ref[out_rows(2 * n + 1 - half), :] = o_in[n].astype(jnp.float32)

    def rows_ready(u):
        n, second = UNITS[u]
        if not second:
            with jax.named_scope("x_last"):
                arrived(rows.at[0, pl.ds(0, 2 * tokens), :], x_recv.at[n, 1])
            turned[min(n, PAIRS)] = rows[chunk_of(n)].T

    def dot(u, place):
        n, second = UNITS[u]
        at_place = pl.ds(pl.multiple_of(place * NC * NB, NC * NB), NC * NB)
        value = jnp.dot(turned[min(n, PAIRS)], cols[second, :, at_place], preferred_element_type=jnp.float32)
        for i in range(NC):
            prod[u, NC * place + i] = value[:, i * NB : (i + 1) * NB]

    def product(u):
        rows_ready(u)
        with jax.named_scope("dot"):
            for place in range(NY):
                dot(u, place)
        first(u)

    def part(u, part):
        if part:
            dot(u, lax.rem(y + 2, NY))
        else:
            rows_ready(u)
            with jax.named_scope("dot"):
                for step in (0, 1, 3):
                    dot(u, lax.rem(y + step, NY))
        pfirst(u, part)

    def load(i):
        return (
            pltpu.make_async_copy(gate_hbm.at[:, lanes(i)], gate_buf.at[i], load_sem.at[i // LOADS]),
            pltpu.make_async_copy(up_hbm.at[:, lanes(i)], up_buf.at[i], load_sem.at[i // LOADS]),
        )

    def hide():
        def one(i, carry):
            gate = gate_buf[i].astype(jnp.float32)
            act = gate / (1.0 + jnp.exp(-gate))
            rows[i, row_block(x), :] = (act * up_buf[i].astype(jnp.float32)).astype(jnp.bfloat16)
            return carry

        for i in range(CHUNKS):
            for copy in load(i):
                copy.start()
        if PAIRS:
            cols[1, row_block(x), lanes(mine)] = grad_buf[lax.rem(x + 2, NX)]
        with jax.named_scope("hide"):
            for group in range(CHUNKS // LOADS):
                both = gate_buf.at[pl.ds(0, 2 * LOADS)]
                pltpu.make_async_copy(both, both, load_sem.at[group]).wait()
                lax.fori_loop(group * LOADS, (group + 1) * LOADS, one, 0)

    partners = (
        at(dz=1), at(dz=-1), at(dz=2), at(dz=-2), at(dx=1), at(dx=-1), at(dx=2), at(dy=1), at(dy=-1), at(dc=1),
    )
    barrier = pltpu.get_barrier_semaphore()
    for device in partners:
        pl.semaphore_signal(barrier, inc=1, device_id=device, device_id_type=MESH)
    grad_copy = [
        pltpu.make_async_copy(grad_hbm.at[:, pl.ds(k * NB, NB)], grad_buf.at[k], grad_sem) for k in range(NX)
    ]
    for copy in grad_copy:
        copy.start()
    with jax.named_scope("grad"):
        pltpu.make_async_copy(grad_buf, grad_buf, grad_sem).wait()
    cols[0, row_block(x), lanes(mine)] = grad_buf[x]
    with jax.named_scope("barrier"):
        pl.semaphore_wait(barrier, len(partners))

    steps = {
        "b_near": b_near, "b_far2": b_far2, "b_own": b_own, "b_take": b_take, "b_pass": b_pass, "b_far": b_far,
        "b_most": b_most, "b_rest": b_rest, "part": part, "pmid": pmid, "plast": last,
        "hide": hide, "x_own": x_own, "x_pass": x_pass, "product": product, "mid": mid, "qmid": qmid, "last": last,
        "o_last": o_last,
    }
    for name, *arguments in ORDER:
        steps[name](*arguments)

    def sent(ref, sem):
        remote(ref, ref, sem, x_recv.at[0, 0], at(dx=1)).wait_send()

    with jax.named_scope("sent"):
        sent(rows.at[pl.ds(0, ITEMS), pl.ds(0, 3 * tokens), :], x_send)
        sets = 2 if PAIRS else 1
        sent(rows.at[pl.ds(0, sets), pl.ds(0, 3 * tokens), :], b_send.at[0])
        sent(rows.at[pl.ds(0, 3 * sets)], b_send.at[1])
        sent(rows.at[pl.ds(0, 4 * sets)], b_send.at[2])
        sent(z_out, z_send)
        if PAIRS:
            sent(o_out, o_send)


def solution(mesh):
    def shards(gate_pre, up_pre, out_grad):
        tokens, hidden = gate_pre.shape
        depth = NX * tokens
        dma = pltpu.SemaphoreType.DMA
        operands = [pltpu.with_memory_space_constraint(a, pltpu.HBM) for a in (gate_pre, up_pre, out_grad)]
        return pl.pallas_call(
            kernel,
            out_shape=jax.ShapeDtypeStruct((hidden, NB), jnp.float32),
            in_specs=[pl.BlockSpec(memory_space=pl.ANY)] * 3,
            out_specs=pl.BlockSpec(memory_space=pltpu.VMEM),
            scratch_shapes=[
                pltpu.VMEM((CHUNKS, tokens, MC), jnp.bfloat16),
                pltpu.VMEM((CHUNKS, tokens, MC), jnp.bfloat16),
                pltpu.VMEM((NX, tokens, NB), jnp.bfloat16),
                pltpu.VMEM((CHUNKS, depth, MC), jnp.bfloat16),
                pltpu.VMEM((PAIRS + 1, MC, depth), jnp.bfloat16),
                pltpu.VMEM((2, depth, NZ * NB), jnp.bfloat16),
                pltpu.VMEM((CHUNKS, NZ, MC, NB), jnp.float32),
                pltpu.VMEM((CHUNKS, 7, MC, NB), jnp.bfloat16),
                pltpu.VMEM((CHUNKS, 7, MC, NB), jnp.bfloat16),
                pltpu.VMEM((max(PAIRS, 1), MC, NB), jnp.bfloat16),
                pltpu.VMEM((max(PAIRS, 1), MC, NB), jnp.bfloat16),
                dma((CHUNKS // LOADS,)),
                dma,
                dma,
                dma((ITEMS, 2)),
                dma((3,)),
                dma((2, 3)),
                dma((2, NX, 2)),
                dma((2, 2)),
                dma,
                dma((4 * CHUNKS + 2 * len(SPLIT),)),
                dma,
                dma((max(PAIRS, 1),)),
            ],
            compiler_params=pltpu.CompilerParams(
                collective_id=0, has_side_effects=True, vmem_limit_bytes=VMEM_BYTES
            ),
        )(*operands)

    return jax.shard_map(
        shards,
        mesh=mesh,
        in_specs=(P("node", "local"), P("node", "local"), P("node", "local")),
        out_specs=P("local", "node"),
        check_vma=False,
    )
```

```python
import jax
import jax.numpy as jnp
from jax import lax
from jax.experimental import pallas as pl
from jax.experimental.pallas import tpu as pltpu
from jax.sharding import PartitionSpec as P

MESH = pl.DeviceIdType.MESH
NZ, NX, NY, NC = 8, 4, 4, 2
MC = 128
LOADS = 5
NB = 128
CHUNKS = 15
PAIRS = 6
ITEMS = CHUNKS - PAIRS
UNITS = [(i, 0) for i in range(PAIRS)] + [(i, 1) for i in range(PAIRS)] + [(i, 0) for i in range(PAIRS, ITEMS)]
SPLIT = (0, 1, 6)
QUICK = 0
VMEM_BYTES = 50_000_000
ORDER = (
    ("b_near", 0), ("b_own", 0, 0), ("hide",), ("b_own", 1, 0), ("b_far2", 0), ("x_own", 0), ("b_own", 0, 1),
    ("x_own", 1), ("b_own", 0, 2), ("b_near", 1), ("b_take", 1, 0), ("x_pass", 0), ("b_far2", 1), ("b_own", 0, 3),
    ("b_take", 0, 1), ("x_pass", 1), ("b_take", 0, 2), ("b_pass", 0, 1), ("b_pass", 0, 2), ("x_own", 2),
    ("b_own", 1, 2), ("b_take", 0, 3), ("b_take", 0, 0), ("b_most", 0), ("b_own", 1, 1), ("b_pass", 0, 3),
    ("b_pass", 0, 0), ("x_own", 3), ("part", 0, 0), ("b_far", 0, 1), ("b_far", 0, 2), ("b_take", 1, 2), ("x_pass", 2),
    ("x_own", 4), ("b_own", 1, 3), ("part", 1, 0), ("b_take", 1, 1), ("x_pass", 3), ("pmid", 0, 1, 0),
    ("b_pass", 1, 2), ("b_far", 0, 0), ("b_pass", 1, 1), ("b_far", 0, 3), ("b_pass", 1, 0), ("x_pass", 4),
    ("b_rest", 0), ("part", 1, 1), ("part", 0, 1), ("pmid", 1, 1, 0), ("b_take", 1, 3), ("x_own", 5),
    ("b_pass", 1, 3), ("pmid", 0, 2, 0), ("product", 2), ("b_most", 1), ("part", 6, 0), ("x_own", 6), ("product", 3),
    ("pmid", 1, 1, 1), ("b_far", 1, 2), ("pmid", 0, 1, 1), ("product", 4), ("pmid", 1, 2, 0), ("b_far", 1, 1),
    ("b_far", 1, 0), ("b_far", 1, 3), ("mid", 2, 1), ("x_pass", 5), ("x_own", 7), ("x_own", 8), ("pmid", 0, 3, 0),
    ("pmid", 6, 1, 0), ("b_rest", 1), ("part", 6, 1), ("product", 8), ("x_pass", 6), ("mid", 3, 1), ("product", 7),
    ("mid", 4, 1), ("product", 10), ("pmid", 1, 2, 1), ("product", 9), ("mid", 8, 1), ("product", 5), ("x_pass", 7),
    ("x_pass", 8), ("mid", 2, 2), ("mid", 10, 1), ("product", 11), ("pmid", 0, 2, 1), ("pmid", 6, 2, 0),
    ("mid", 9, 1), ("mid", 7, 1), ("mid", 5, 1), ("pmid", 6, 1, 1), ("product", 12), ("mid", 11, 1), ("mid", 8, 2),
    ("product", 14), ("product", 13), ("mid", 7, 2), ("pmid", 6, 2, 1), ("mid", 10, 2), ("mid", 9, 2), ("mid", 12, 1),
    ("mid", 11, 2), ("pmid", 0, 3, 1), ("mid", 3, 2), ("mid", 14, 1), ("pmid", 6, 3, 1), ("mid", 13, 1),
    ("mid", 7, 3), ("mid", 9, 3), ("mid", 5, 2), ("mid", 8, 3), ("pmid", 6, 3, 0), ("mid", 10, 3), ("mid", 11, 3),
    ("mid", 4, 2), ("mid", 14, 2), ("mid", 12, 2), ("mid", 13, 2), ("mid", 3, 3), ("pmid", 1, 3, 0), ("last", 7),
    ("last", 9), ("last", 8), ("plast", 6), ("pmid", 1, 3, 1), ("mid", 5, 3), ("last", 11), ("mid", 2, 3),
    ("last", 10), ("mid", 4, 3), ("mid", 14, 3), ("mid", 12, 3), ("mid", 13, 3), ("last", 5), ("last", 4),
    ("last", 2), ("o_last", 1), ("plast", 1), ("o_last", 0), ("last", 3), ("o_last", 5), ("o_last", 2), ("last", 14),
    ("o_last", 3), ("last", 12), ("o_last", 4), ("plast", 0), ("last", 13),
)


def kernel(
    gate_hbm, up_hbm, grad_hbm, out_ref,
    gate_buf, up_buf, grad_buf, rows, turned, cols, prod, z_out, z_in, o_out, o_in,
    load_sem, grad_sem, x_send, x_recv, b_send, bx_recv, by_recv, bs_recv, z_send, z_recv, o_send, o_recv,
):
    tokens = grad_hbm.shape[0]
    node, local = lax.axis_index("node"), lax.axis_index("local")
    z, x = node // NX, node % NX
    y, core = local // NC, local % NC
    mine = y * NC + core

    def at(dz=0, dx=0, dy=0, dc=0):
        return {
            "node": lax.rem(z + dz + NZ, NZ) * NX + lax.rem(x + dx + NX, NX),
            "local": lax.rem(y + dy + NY, NY) * NC + lax.rem(core + dc, NC),
        }

    def remote(src, dst, send, recv, device):
        return pltpu.make_async_remote_copy(
            src_ref=src, dst_ref=dst, send_sem=send, recv_sem=recv, device_id=device, device_id_type=MESH
        )

    def arrived(ref, sem):
        remote(ref, ref, x_send, sem, at(dx=1)).wait_recv()

    def lanes(block):
        return pl.ds(pl.multiple_of(block * NB, NB), NB)

    def row_block(who):
        return pl.ds(pl.multiple_of(who * tokens, tokens), tokens)

    x_of = (x, lax.rem(x + NX - 1, NX), lax.rem(x + 1, NX), lax.rem(x + 2, NX))

    def piece(n, k, block):
        return cols.at[n, row_block(x_of[k]), lanes(block)]

    below = lax.rem(y + NY - 1, NY) * NC + core
    above = lax.rem(y + 1, NY) * NC + core
    across = lax.rem(y + 2, NY) * NC + core

    def b_send_to(n, k, dx):
        block = lax.rem(x + dx + 2 * n + NX, NX)
        remote(grad_buf.at[block], piece(n, 0, mine), b_send.at[0], bx_recv.at[n, k], at(dx=dx)).start()

    def b_near(n):
        b_send_to(n, 0, 1)
        b_send_to(n, 1, -1)

    def b_far2(n):
        b_send_to(n, 2, 2)

    def b_along(n, k, block, sem, dy):
        remote(piece(n, k, block), piece(n, k, block), b_send.at[1], sem, at(dy=dy)).start()

    def b_over(n, k, block, part=0):
        remote(piece(n, k, block), piece(n, k, block), b_send.at[2], bs_recv.at[n, part], at(dc=1)).start()

    def b_own(n, k):
        if k:
            with jax.named_scope(f"bx_{n}{k}"):
                arrived(grad_buf.at[0], bx_recv.at[n, k - 1])
        b_along(n, k, mine, by_recv.at[n, k, 0], 1)
        b_along(n, k, mine, by_recv.at[n, k, 0], -1)
        b_over(n, k, mine)

    def b_take(n, k):
        with jax.named_scope(f"by_{n}{k}"):
            arrived(rows.at[0, pl.ds(0, 2 * tokens), :], by_recv.at[n, k, 0])
        b_over(n, k, below)
        b_over(n, k, above)

    def b_pass(n, k):
        up = lax.rem(core + k, 2) == 0
        b_along(n, k, jnp.where(up, below, above), by_recv.at[n, k, 1], jnp.where(up, 1, -1))

    def b_far(n, k):
        with jax.named_scope(f"bf_{n}{k}"):
            arrived(grad_buf.at[0], by_recv.at[n, k, 1])
        b_over(n, k, across, 1)

    def b_most(n):
        with jax.named_scope(f"bm_{n}"):
            arrived(rows.at[pl.ds(0, 3)], bs_recv.at[n, 0])

    def b_rest(n):
        with jax.named_scope(f"br_{n}"):
            arrived(rows.at[0], bs_recv.at[n, 1])

    def rows_of(i, who):
        return rows.at[i, row_block(who), :]

    pair_step = 1 - 2 * lax.rem(x + core, 2)
    half = lax.rem(x - core + NX, NX) // 2

    def chunk_of(n):
        return 2 * n + half if n < PAIRS else n + PAIRS

    def step_of(n):
        return pair_step if n < PAIRS or n % 2 == 0 else -pair_step

    def x_own(n):
        mine_of, other = chunk_of(n), 2 * n + 1 - half if n < PAIRS else chunk_of(n)
        remote(rows_of(other, x), rows_of(other, x), x_send, x_recv.at[n, 0], at(dx=-step_of(n))).start()
        remote(rows_of(mine_of, x), rows_of(mine_of, x), x_send, x_recv.at[n, 1], at(dx=step_of(n))).start()

    def x_pass(n):
        with jax.named_scope("x_pass"):
            arrived(rows_of(0, x), x_recv.at[n, 0])
        block = rows_of(chunk_of(n), lax.rem(x - step_of(n) + NX, NX))
        remote(block, block, x_send, x_recv.at[n, 1], at(dx=step_of(n))).start()

    sign = 2 * core - 1

    def z_sem(u, sem):
        return z_recv.at[4 * u + 2 * sum(v < u for v in SPLIT) + sem]

    def z_move(u, slot, hop, sem):
        remote(z_out.at[u, slot], z_in.at[u, slot], z_send, z_sem(u, sem), at(dz=hop * sign)).start()

    def z_wait(u, count, sem):
        with jax.named_scope(f"z_{sem}"):
            arrived(z_in.at[u, pl.ds(0, count)], z_sem(u, sem))

    def block_at(offset):
        return lax.rem(z + offset * sign + NZ, NZ)

    def z_put(u, slot, offset, *added):
        value = prod[u, block_at(offset)]
        for other in added:
            value = value + z_in[u, other].astype(jnp.float32)
        z_out[u, slot] = value.astype(jnp.bfloat16)

    def is_quick(u):
        return u >= CHUNKS - QUICK

    def first(u):
        if is_quick(u):
            moves = ((0, 4, 2, 0), (4, -3, -2, 0), (1, 3, 1, 0), (5, -2, -1, 0), (3, 1, 1, 3))
        else:
            moves = ((0, 4, 1, 0), (4, -3, -1, 0))
        for slot, offset, hop, sem in moves:
            z_put(u, slot, offset)
            z_move(u, slot, hop, sem)

    def mid(u, s):
        z_wait(u, 2 if s < 3 else 1, s - 1)
        z_put(u, s, 4 - s, s - 1)
        z_move(u, s, 1, s if s < 3 else 3)
        if s < 3:
            z_put(u, 4 + s, s - 3, 3 + s)
            z_move(u, 4 + s, -1, s if s < 2 else 3)

    def qmid(u):
        z_wait(u, 4, 0)
        z_put(u, 2, 2, 0, 1)
        z_move(u, 2, 2, 3)
        z_put(u, 6, -1, 4, 5)
        z_move(u, 6, -1, 3)

    def if_part(offset, part, body):
        far = block_at(offset) // NC == lax.rem(y + 2, NY)
        pl.when(far if part else jnp.logical_not(far))(body)

    def pfirst(u, part):
        for slot, offset, hop, sem in ((0, 4, 1, 0), (4, -3, -1, 4)):
            def body(slot=slot, offset=offset, hop=hop, sem=sem):
                z_put(u, slot, offset)
                z_move(u, slot, hop, sem)
            if_part(offset, part, body)

    def pmid(u, s, part):
        def long():
            z_wait(u, 1, s - 1)
            z_put(u, s, 4 - s, s - 1)
            z_move(u, s, 1, s)

        def short():
            z_wait(u, 1, 3 + s)
            z_put(u, 4 + s, s - 3, 3 + s)
            z_move(u, 4 + s, -1, 4 + s if s < 2 else 3)

        if_part(4 - s, part, long)
        if s < 3:
            if_part(s - 3, part, short)

    def out_rows(chunk):
        return pl.ds(pl.multiple_of(chunk * MC, MC), MC)

    def last(u):
        added = (2, 3, 6) if is_quick(u) else (3, 6)
        z_wait(u, len(added), 3)
        value = prod[u, z]
        for other in added:
            value = value + z_in[u, other].astype(jnp.float32)
        value = value * (1.0 / (NZ * NX))
        n, second = UNITS[u]
        if second:
            o_out[n] = value.astype(jnp.bfloat16)
            remote(o_out.at[n], o_in.at[n], o_send, o_recv.at[n], at(dx=2)).start()
        else:
            out_ref[out_rows(chunk_of(n)), :] = value

    def o_last(n):
        with jax.named_scope("o"):
            arrived(o_in.at[0], o_recv.at[n])
        out_ref[out_rows(2 * n + 1 - half), :] = o_in[n].astype(jnp.float32)

    def rows_ready(u):
        n, second = UNITS[u]
        if not second:
            with jax.named_scope("x_last"):
                arrived(rows.at[0, pl.ds(0, 2 * tokens), :], x_recv.at[n, 1])
            turned[min(n, PAIRS)] = rows[chunk_of(n)].T

    def dot(u, place):
        n, second = UNITS[u]
        at_place = pl.ds(pl.multiple_of(place * NC * NB, NC * NB), NC * NB)
        value = jnp.dot(turned[min(n, PAIRS)], cols[second, :, at_place], preferred_element_type=jnp.float32)
        for i in range(NC):
            prod[u, NC * place + i] = value[:, i * NB : (i + 1) * NB]

    def product(u):
        rows_ready(u)
        with jax.named_scope("dot"):
            for place in range(NY):
                dot(u, place)
        first(u)

    def part(u, part):
        if part:
            dot(u, lax.rem(y + 2, NY))
        else:
            rows_ready(u)
            with jax.named_scope("dot"):
                for step in (0, 1, 3):
                    dot(u, lax.rem(y + step, NY))
        pfirst(u, part)

    def load(i):
        return (
            pltpu.make_async_copy(gate_hbm.at[:, lanes(i)], gate_buf.at[i], load_sem.at[i // LOADS]),
            pltpu.make_async_copy(up_hbm.at[:, lanes(i)], up_buf.at[i], load_sem.at[i // LOADS]),
        )

    def hide():
        def one(i, carry):
            gate = gate_buf[i].astype(jnp.float32)
            act = gate / (1.0 + jnp.exp(-gate))
            rows[i, row_block(x), :] = (act * up_buf[i].astype(jnp.float32)).astype(jnp.bfloat16)
            return carry

        for i in range(CHUNKS):
            for copy in load(i):
                copy.start()
        if PAIRS:
            cols[1, row_block(x), lanes(mine)] = grad_buf[lax.rem(x + 2, NX)]
        with jax.named_scope("hide"):
            for group in range(CHUNKS // LOADS):
                both = gate_buf.at[pl.ds(0, 2 * LOADS)]
                pltpu.make_async_copy(both, both, load_sem.at[group]).wait()
                lax.fori_loop(group * LOADS, (group + 1) * LOADS, one, 0)

    partners = (
        at(dz=1), at(dz=-1), at(dx=1), at(dx=-1), at(dx=2), at(dy=1), at(dy=-1), at(dc=1),
    )
    if QUICK:
        partners += (at(dz=2), at(dz=-2))
    barrier = pltpu.get_barrier_semaphore()
    for device in partners:
        pl.semaphore_signal(barrier, inc=1, device_id=device, device_id_type=MESH)
    grad_copy = [
        pltpu.make_async_copy(grad_hbm.at[:, pl.ds(k * NB, NB)], grad_buf.at[k], grad_sem) for k in range(NX)
    ]
    for copy in grad_copy:
        copy.start()
    with jax.named_scope("grad"):
        pltpu.make_async_copy(grad_buf, grad_buf, grad_sem).wait()
    cols[0, row_block(x), lanes(mine)] = grad_buf[x]
    with jax.named_scope("barrier"):
        pl.semaphore_wait(barrier, len(partners))

    steps = {
        "b_near": b_near, "b_far2": b_far2, "b_own": b_own, "b_take": b_take, "b_pass": b_pass, "b_far": b_far,
        "b_most": b_most, "b_rest": b_rest, "part": part, "pmid": pmid, "plast": last,
        "hide": hide, "x_own": x_own, "x_pass": x_pass, "product": product, "mid": mid, "qmid": qmid, "last": last,
        "o_last": o_last,
    }
    for name, *arguments in ORDER:
        steps[name](*arguments)

    def sent(ref, sem):
        remote(ref, ref, sem, x_recv.at[0, 0], at(dx=1)).wait_send()

    with jax.named_scope("sent"):
        sent(rows.at[pl.ds(0, ITEMS), pl.ds(0, 3 * tokens), :], x_send)
        sets = 2 if PAIRS else 1
        sent(rows.at[pl.ds(0, sets), pl.ds(0, 3 * tokens), :], b_send.at[0])
        sent(rows.at[pl.ds(0, 3 * sets)], b_send.at[1])
        sent(rows.at[pl.ds(0, 4 * sets)], b_send.at[2])
        sent(z_out, z_send)
        if PAIRS:
            sent(o_out, o_send)


def solution(mesh):
    def shards(gate_pre, up_pre, out_grad):
        tokens, hidden = gate_pre.shape
        depth = NX * tokens
        dma = pltpu.SemaphoreType.DMA
        operands = [pltpu.with_memory_space_constraint(a, pltpu.HBM) for a in (gate_pre, up_pre, out_grad)]
        return pl.pallas_call(
            kernel,
            out_shape=jax.ShapeDtypeStruct((hidden, NB), jnp.float32),
            in_specs=[pl.BlockSpec(memory_space=pl.ANY)] * 3,
            out_specs=pl.BlockSpec(memory_space=pltpu.VMEM),
            scratch_shapes=[
                pltpu.VMEM((CHUNKS, tokens, MC), jnp.bfloat16),
                pltpu.VMEM((CHUNKS, tokens, MC), jnp.bfloat16),
                pltpu.VMEM((NX, tokens, NB), jnp.bfloat16),
                pltpu.VMEM((CHUNKS, depth, MC), jnp.bfloat16),
                pltpu.VMEM((PAIRS + 1, MC, depth), jnp.bfloat16),
                pltpu.VMEM((2, depth, NZ * NB), jnp.bfloat16),
                pltpu.VMEM((CHUNKS, NZ, MC, NB), jnp.float32),
                pltpu.VMEM((CHUNKS, 7, MC, NB), jnp.bfloat16),
                pltpu.VMEM((CHUNKS, 7, MC, NB), jnp.bfloat16),
                pltpu.VMEM((max(PAIRS, 1), MC, NB), jnp.bfloat16),
                pltpu.VMEM((max(PAIRS, 1), MC, NB), jnp.bfloat16),
                dma((CHUNKS // LOADS,)),
                dma,
                dma,
                dma((ITEMS, 2)),
                dma((3,)),
                dma((2, 3)),
                dma((2, NX, 2)),
                dma((2, 2)),
                dma,
                dma((4 * CHUNKS + 2 * len(SPLIT),)),
                dma,
                dma((max(PAIRS, 1),)),
            ],
            compiler_params=pltpu.CompilerParams(
                collective_id=0, has_side_effects=True, vmem_limit_bytes=VMEM_BYTES
            ),
        )(*operands)

    return jax.shard_map(
        shards,
        mesh=mesh,
        in_specs=(P("node", "local"), P("node", "local"), P("node", "local")),
        out_specs=P("local", "node"),
        check_vma=False,
    )
```

```python
import jax
import jax.numpy as jnp
from jax import lax
from jax.experimental import pallas as pl
from jax.experimental.pallas import tpu as pltpu
from jax.sharding import PartitionSpec as P

MESH = pl.DeviceIdType.MESH
NZ, NX, NY, NC = 8, 4, 4, 2
MC = 128
LOADS = 5
NB = 128
CHUNKS = 15
PAIRS = 6
ITEMS = CHUNKS - PAIRS
UNITS = [(i, 0) for i in range(PAIRS)] + [(i, 1) for i in range(PAIRS)] + [(i, 0) for i in range(PAIRS, ITEMS)]
SPLIT = (0, 1, 6)
QUICK = 0
VMEM_BYTES = 50_000_000
ORDER = (
    ("b_near", 0), ("b_own", 0, 0), ("b_own", 1, 0), ("hide",), ("b_far2", 0), ("x_own", 0), ("b_own", 0, 1),
    ("x_own", 1), ("b_own", 0, 2), ("b_near", 1), ("b_take", 1, 0), ("x_pass", 0), ("b_far2", 1), ("b_own", 0, 3),
    ("b_take", 0, 1), ("x_pass", 1), ("b_take", 0, 2), ("b_pass", 0, 1), ("b_pass", 0, 2), ("x_own", 2),
    ("b_own", 1, 2), ("b_take", 0, 3), ("b_take", 0, 0), ("b_most", 0), ("b_own", 1, 1), ("b_pass", 0, 3),
    ("b_pass", 0, 0), ("x_own", 3), ("part", 0, 0), ("b_far", 0, 1), ("b_far", 0, 2), ("b_take", 1, 2), ("x_pass", 2),
    ("x_own", 4), ("b_own", 1, 3), ("part", 1, 0), ("b_take", 1, 1), ("x_pass", 3), ("pmid", 0, 1, 0),
    ("b_pass", 1, 2), ("b_far", 0, 0), ("b_pass", 1, 1), ("b_far", 0, 3), ("b_pass", 1, 0), ("x_pass", 4),
    ("b_rest", 0), ("part", 1, 1), ("part", 0, 1), ("pmid", 1, 1, 0), ("b_take", 1, 3), ("x_own", 5),
    ("b_pass", 1, 3), ("pmid", 0, 2, 0), ("product", 2), ("b_most", 1), ("part", 6, 0), ("x_own", 6), ("product", 3),
    ("pmid", 1, 1, 1), ("b_far", 1, 2), ("pmid", 0, 1, 1), ("product", 4), ("pmid", 1, 2, 0), ("b_far", 1, 1),
    ("b_far", 1, 0), ("b_far", 1, 3), ("mid", 2, 1), ("x_pass", 5), ("x_own", 7), ("x_own", 8), ("pmid", 0, 3, 0),
    ("pmid", 6, 1, 0), ("b_rest", 1), ("part", 6, 1), ("product", 8), ("x_pass", 6), ("mid", 3, 1), ("product", 7),
    ("mid", 4, 1), ("product", 10), ("pmid", 1, 2, 1), ("product", 9), ("mid", 8, 1), ("product", 5), ("x_pass", 7),
    ("x_pass", 8), ("mid", 2, 2), ("mid", 10, 1), ("product", 11), ("pmid", 0, 2, 1), ("pmid", 6, 2, 0),
    ("mid", 9, 1), ("mid", 7, 1), ("mid", 5, 1), ("pmid", 6, 1, 1), ("product", 12), ("mid", 11, 1), ("mid", 8, 2),
    ("product", 14), ("product", 13), ("mid", 7, 2), ("pmid", 6, 2, 1), ("mid", 10, 2), ("mid", 9, 2), ("mid", 12, 1),
    ("mid", 11, 2), ("pmid", 0, 3, 1), ("mid", 3, 2), ("mid", 14, 1), ("pmid", 6, 3, 1), ("mid", 13, 1),
    ("mid", 7, 3), ("mid", 9, 3), ("mid", 5, 2), ("mid", 8, 3), ("pmid", 6, 3, 0), ("mid", 10, 3), ("mid", 11, 3),
    ("mid", 4, 2), ("mid", 14, 2), ("mid", 12, 2), ("mid", 13, 2), ("mid", 3, 3), ("pmid", 1, 3, 0), ("last", 7),
    ("last", 9), ("last", 8), ("plast", 6), ("pmid", 1, 3, 1), ("mid", 5, 3), ("last", 11), ("mid", 2, 3),
    ("last", 10), ("mid", 4, 3), ("mid", 14, 3), ("mid", 12, 3), ("mid", 13, 3), ("last", 5), ("last", 4),
    ("last", 2), ("o_last", 1), ("plast", 1), ("o_last", 0), ("last", 3), ("o_last", 5), ("o_last", 2), ("last", 14),
    ("o_last", 3), ("last", 12), ("o_last", 4), ("plast", 0), ("last", 13),
)


def kernel(
    gate_hbm, up_hbm, grad_hbm, out_ref,
    gate_buf, up_buf, grad_buf, rows, turned, cols, prod, z_out, z_in, o_out, o_in,
    load_sem, grad_sem, x_send, x_recv, b_send, bx_recv, by_recv, bs_recv, z_send, z_recv, o_send, o_recv,
):
    tokens = grad_hbm.shape[0]
    node, local = lax.axis_index("node"), lax.axis_index("local")
    z, x = node // NX, node % NX
    y, core = local // NC, local % NC
    mine = y * NC + core

    def at(dz=0, dx=0, dy=0, dc=0):
        return {
            "node": lax.rem(z + dz + NZ, NZ) * NX + lax.rem(x + dx + NX, NX),
            "local": lax.rem(y + dy + NY, NY) * NC + lax.rem(core + dc, NC),
        }

    def remote(src, dst, send, recv, device):
        return pltpu.make_async_remote_copy(
            src_ref=src, dst_ref=dst, send_sem=send, recv_sem=recv, device_id=device, device_id_type=MESH
        )

    def arrived(ref, sem):
        remote(ref, ref, x_send, sem, at(dx=1)).wait_recv()

    def lanes(block):
        return pl.ds(pl.multiple_of(block * NB, NB), NB)

    def row_block(who):
        return pl.ds(pl.multiple_of(who * tokens, tokens), tokens)

    x_of = (x, lax.rem(x + NX - 1, NX), lax.rem(x + 1, NX), lax.rem(x + 2, NX))

    def piece(n, k, block):
        return cols.at[n, row_block(x_of[k]), lanes(block)]

    below = lax.rem(y + NY - 1, NY) * NC + core
    above = lax.rem(y + 1, NY) * NC + core
    across = lax.rem(y + 2, NY) * NC + core

    def b_send_to(n, k, dx):
        block = lax.rem(x + dx + 2 * n + NX, NX)
        remote(grad_buf.at[block], piece(n, 0, mine), b_send.at[0], bx_recv.at[n, k], at(dx=dx)).start()

    def b_near(n):
        b_send_to(n, 0, 1)
        b_send_to(n, 1, -1)

    def b_far2(n):
        b_send_to(n, 2, 2)

    def held(n, k, block, own):
        return grad_buf.at[lax.rem(x + 2 * n, NX)] if own and k == 0 else piece(n, k, block)

    def b_along(n, k, block, sem, dy, own=False):
        remote(held(n, k, block, own), piece(n, k, block), b_send.at[1], sem, at(dy=dy)).start()

    def b_over(n, k, block, part=0, own=False):
        remote(held(n, k, block, own), piece(n, k, block), b_send.at[2], bs_recv.at[n, part], at(dc=1)).start()

    def b_own(n, k):
        if k:
            with jax.named_scope(f"bx_{n}{k}"):
                arrived(grad_buf.at[0], bx_recv.at[n, k - 1])
        b_along(n, k, mine, by_recv.at[n, k, 0], 1, own=True)
        b_along(n, k, mine, by_recv.at[n, k, 0], -1, own=True)
        b_over(n, k, mine, own=True)

    def b_take(n, k):
        with jax.named_scope(f"by_{n}{k}"):
            arrived(rows.at[0, pl.ds(0, 2 * tokens), :], by_recv.at[n, k, 0])
        b_over(n, k, below)
        b_over(n, k, above)

    def b_pass(n, k):
        up = lax.rem(core + k, 2) == 0
        b_along(n, k, jnp.where(up, below, above), by_recv.at[n, k, 1], jnp.where(up, 1, -1))

    def b_far(n, k):
        with jax.named_scope(f"bf_{n}{k}"):
            arrived(grad_buf.at[0], by_recv.at[n, k, 1])
        b_over(n, k, across, 1)

    def b_most(n):
        with jax.named_scope(f"bm_{n}"):
            arrived(rows.at[pl.ds(0, 3)], bs_recv.at[n, 0])

    def b_rest(n):
        with jax.named_scope(f"br_{n}"):
            arrived(rows.at[0], bs_recv.at[n, 1])

    def rows_of(i, who):
        return rows.at[i, row_block(who), :]

    pair_step = 1 - 2 * lax.rem(x + core, 2)
    half = lax.rem(x - core + NX, NX) // 2

    def chunk_of(n):
        return 2 * n + half if n < PAIRS else n + PAIRS

    def step_of(n):
        return pair_step if n < PAIRS or n % 2 == 0 else -pair_step

    def x_own(n):
        mine_of, other = chunk_of(n), 2 * n + 1 - half if n < PAIRS else chunk_of(n)
        remote(rows_of(other, x), rows_of(other, x), x_send, x_recv.at[n, 0], at(dx=-step_of(n))).start()
        remote(rows_of(mine_of, x), rows_of(mine_of, x), x_send, x_recv.at[n, 1], at(dx=step_of(n))).start()

    def x_pass(n):
        with jax.named_scope("x_pass"):
            arrived(rows_of(0, x), x_recv.at[n, 0])
        block = rows_of(chunk_of(n), lax.rem(x - step_of(n) + NX, NX))
        remote(block, block, x_send, x_recv.at[n, 1], at(dx=step_of(n))).start()

    sign = 2 * core - 1

    def z_sem(u, sem):
        return z_recv.at[4 * u + 2 * sum(v < u for v in SPLIT) + sem]

    def z_move(u, slot, hop, sem):
        remote(z_out.at[u, slot], z_in.at[u, slot], z_send, z_sem(u, sem), at(dz=hop * sign)).start()

    def z_wait(u, count, sem):
        with jax.named_scope(f"z_{sem}"):
            arrived(z_in.at[u, pl.ds(0, count)], z_sem(u, sem))

    def block_at(offset):
        return lax.rem(z + offset * sign + NZ, NZ)

    def z_put(u, slot, offset, *added):
        value = prod[u, block_at(offset)]
        for other in added:
            value = value + z_in[u, other].astype(jnp.float32)
        z_out[u, slot] = value.astype(jnp.bfloat16)

    def is_quick(u):
        return u >= CHUNKS - QUICK

    def first(u):
        if is_quick(u):
            moves = ((0, 4, 2, 0), (4, -3, -2, 0), (1, 3, 1, 0), (5, -2, -1, 0), (3, 1, 1, 3))
        else:
            moves = ((0, 4, 1, 0), (4, -3, -1, 0))
        for slot, offset, hop, sem in moves:
            z_put(u, slot, offset)
            z_move(u, slot, hop, sem)

    def mid(u, s):
        z_wait(u, 2 if s < 3 else 1, s - 1)
        z_put(u, s, 4 - s, s - 1)
        z_move(u, s, 1, s if s < 3 else 3)
        if s < 3:
            z_put(u, 4 + s, s - 3, 3 + s)
            z_move(u, 4 + s, -1, s if s < 2 else 3)

    def qmid(u):
        z_wait(u, 4, 0)
        z_put(u, 2, 2, 0, 1)
        z_move(u, 2, 2, 3)
        z_put(u, 6, -1, 4, 5)
        z_move(u, 6, -1, 3)

    def if_part(offset, part, body):
        far = block_at(offset) // NC == lax.rem(y + 2, NY)
        pl.when(far if part else jnp.logical_not(far))(body)

    def pfirst(u, part):
        for slot, offset, hop, sem in ((0, 4, 1, 0), (4, -3, -1, 4)):
            def body(slot=slot, offset=offset, hop=hop, sem=sem):
                z_put(u, slot, offset)
                z_move(u, slot, hop, sem)
            if_part(offset, part, body)

    def pmid(u, s, part):
        def long():
            z_wait(u, 1, s - 1)
            z_put(u, s, 4 - s, s - 1)
            z_move(u, s, 1, s)

        def short():
            z_wait(u, 1, 3 + s)
            z_put(u, 4 + s, s - 3, 3 + s)
            z_move(u, 4 + s, -1, 4 + s if s < 2 else 3)

        if_part(4 - s, part, long)
        if s < 3:
            if_part(s - 3, part, short)

    def out_rows(chunk):
        return pl.ds(pl.multiple_of(chunk * MC, MC), MC)

    def last(u):
        added = (2, 3, 6) if is_quick(u) else (3, 6)
        z_wait(u, len(added), 3)
        value = prod[u, z]
        for other in added:
            value = value + z_in[u, other].astype(jnp.float32)
        value = value * (1.0 / (NZ * NX))
        n, second = UNITS[u]
        if second:
            o_out[n] = value.astype(jnp.bfloat16)
            remote(o_out.at[n], o_in.at[n], o_send, o_recv.at[n], at(dx=2)).start()
        else:
            out_ref[out_rows(chunk_of(n)), :] = value

    def o_last(n):
        with jax.named_scope("o"):
            arrived(o_in.at[0], o_recv.at[n])
        out_ref[out_rows(2 * n + 1 - half), :] = o_in[n].astype(jnp.float32)

    def rows_ready(u):
        n, second = UNITS[u]
        if not second:
            with jax.named_scope("x_last"):
                arrived(rows.at[0, pl.ds(0, 2 * tokens), :], x_recv.at[n, 1])
            turned[min(n, PAIRS)] = rows[chunk_of(n)].T

    def dot(u, place):
        n, second = UNITS[u]
        at_place = pl.ds(pl.multiple_of(place * NC * NB, NC * NB), NC * NB)
        value = jnp.dot(turned[min(n, PAIRS)], cols[second, :, at_place], preferred_element_type=jnp.float32)
        for i in range(NC):
            prod[u, NC * place + i] = value[:, i * NB : (i + 1) * NB]

    def product(u):
        rows_ready(u)
        with jax.named_scope("dot"):
            for place in range(NY):
                dot(u, place)
        first(u)

    def part(u, part):
        if part:
            dot(u, lax.rem(y + 2, NY))
        else:
            rows_ready(u)
            with jax.named_scope("dot"):
                for step in (0, 1, 3):
                    dot(u, lax.rem(y + step, NY))
        pfirst(u, part)

    def load(i):
        return (
            pltpu.make_async_copy(gate_hbm.at[:, lanes(i)], gate_buf.at[i], load_sem.at[i // LOADS]),
            pltpu.make_async_copy(up_hbm.at[:, lanes(i)], up_buf.at[i], load_sem.at[i // LOADS]),
        )

    def hide():
        def one(i, carry):
            gate = gate_buf[i].astype(jnp.float32)
            act = gate / (1.0 + jnp.exp(-gate))
            rows[i, row_block(x), :] = (act * up_buf[i].astype(jnp.float32)).astype(jnp.bfloat16)
            return carry

        for i in range(CHUNKS):
            for copy in load(i):
                copy.start()
        for n in range(2 if PAIRS else 1):
            cols[n, row_block(x), lanes(mine)] = grad_buf[lax.rem(x + 2 * n, NX)]
        with jax.named_scope("hide"):
            for group in range(CHUNKS // LOADS):
                both = gate_buf.at[pl.ds(0, 2 * LOADS)]
                pltpu.make_async_copy(both, both, load_sem.at[group]).wait()
                lax.fori_loop(group * LOADS, (group + 1) * LOADS, one, 0)

    partners = (
        at(dz=1), at(dz=-1), at(dx=1), at(dx=-1), at(dx=2), at(dy=1), at(dy=-1), at(dc=1),
    )
    if QUICK:
        partners += (at(dz=2), at(dz=-2))
    barrier = pltpu.get_barrier_semaphore()
    for device in partners:
        pl.semaphore_signal(barrier, inc=1, device_id=device, device_id_type=MESH)
    grad_copy = [
        pltpu.make_async_copy(grad_hbm.at[:, pl.ds(k * NB, NB)], grad_buf.at[k], grad_sem) for k in range(NX)
    ]
    for copy in grad_copy:
        copy.start()
    with jax.named_scope("grad"):
        pltpu.make_async_copy(grad_buf, grad_buf, grad_sem).wait()
    with jax.named_scope("barrier"):
        pl.semaphore_wait(barrier, len(partners))

    steps = {
        "b_near": b_near, "b_far2": b_far2, "b_own": b_own, "b_take": b_take, "b_pass": b_pass, "b_far": b_far,
        "b_most": b_most, "b_rest": b_rest, "part": part, "pmid": pmid, "plast": last,
        "hide": hide, "x_own": x_own, "x_pass": x_pass, "product": product, "mid": mid, "qmid": qmid, "last": last,
        "o_last": o_last,
    }
    for name, *arguments in ORDER:
        steps[name](*arguments)

    def sent(ref, sem):
        remote(ref, ref, sem, x_recv.at[0, 0], at(dx=1)).wait_send()

    with jax.named_scope("sent"):
        sent(rows.at[pl.ds(0, ITEMS), pl.ds(0, 3 * tokens), :], x_send)
        sets = 2 if PAIRS else 1
        sent(rows.at[pl.ds(0, sets), pl.ds(0, 3 * tokens), :], b_send.at[0])
        sent(rows.at[pl.ds(0, 3 * sets)], b_send.at[1])
        sent(rows.at[pl.ds(0, 4 * sets)], b_send.at[2])
        sent(z_out, z_send)
        if PAIRS:
            sent(o_out, o_send)


def solution(mesh):
    def shards(gate_pre, up_pre, out_grad):
        tokens, hidden = gate_pre.shape
        depth = NX * tokens
        dma = pltpu.SemaphoreType.DMA
        operands = [pltpu.with_memory_space_constraint(a, pltpu.HBM) for a in (gate_pre, up_pre, out_grad)]
        return pl.pallas_call(
            kernel,
            out_shape=jax.ShapeDtypeStruct((hidden, NB), jnp.float32),
            in_specs=[pl.BlockSpec(memory_space=pl.ANY)] * 3,
            out_specs=pl.BlockSpec(memory_space=pltpu.VMEM),
            scratch_shapes=[
                pltpu.VMEM((CHUNKS, tokens, MC), jnp.bfloat16),
                pltpu.VMEM((CHUNKS, tokens, MC), jnp.bfloat16),
                pltpu.VMEM((NX, tokens, NB), jnp.bfloat16),
                pltpu.VMEM((CHUNKS, depth, MC), jnp.bfloat16),
                pltpu.VMEM((PAIRS + 1, MC, depth), jnp.bfloat16),
                pltpu.VMEM((2, depth, NZ * NB), jnp.bfloat16),
                pltpu.VMEM((CHUNKS, NZ, MC, NB), jnp.float32),
                pltpu.VMEM((CHUNKS, 7, MC, NB), jnp.bfloat16),
                pltpu.VMEM((CHUNKS, 7, MC, NB), jnp.bfloat16),
                pltpu.VMEM((max(PAIRS, 1), MC, NB), jnp.bfloat16),
                pltpu.VMEM((max(PAIRS, 1), MC, NB), jnp.bfloat16),
                dma((CHUNKS // LOADS,)),
                dma,
                dma,
                dma((ITEMS, 2)),
                dma((3,)),
                dma((2, 3)),
                dma((2, NX, 2)),
                dma((2, 2)),
                dma,
                dma((4 * CHUNKS + 2 * len(SPLIT),)),
                dma,
                dma((max(PAIRS, 1),)),
            ],
            compiler_params=pltpu.CompilerParams(
                collective_id=0, has_side_effects=True, vmem_limit_bytes=VMEM_BYTES
            ),
        )(*operands)

    return jax.shard_map(
        shards,
        mesh=mesh,
        in_specs=(P("node", "local"), P("node", "local"), P("node", "local")),
        out_specs=P("local", "node"),
        check_vma=False,
    )
```

```python
import jax
import jax.numpy as jnp
from jax import lax
from jax.experimental import pallas as pl
from jax.experimental.pallas import tpu as pltpu
from jax.sharding import PartitionSpec as P

MESH = pl.DeviceIdType.MESH
NZ, NX, NY, NC = 8, 4, 4, 2
MC = 128
LOADS = 3
NB = 128
CHUNKS = 15
PAIRS = 6
ITEMS = CHUNKS - PAIRS
UNITS = [(i, 0) for i in range(PAIRS)] + [(i, 1) for i in range(PAIRS)] + [(i, 0) for i in range(PAIRS, ITEMS)]
SPLIT = (0, 1, 6)
QUICK = 0
VMEM_BYTES = 50_000_000
ORDER = (
    ("b_near", 0), ("b_own", 0, 0), ("b_own", 1, 0), ("hide",), ("b_far2", 0), ("x_own", 0), ("b_own", 0, 1),
    ("x_own", 1), ("b_own", 0, 2), ("b_near", 1), ("b_take", 1, 0), ("x_pass", 0), ("b_far2", 1), ("b_own", 0, 3),
    ("b_take", 0, 1), ("x_pass", 1), ("b_take", 0, 2), ("b_pass", 0, 1), ("b_pass", 0, 2), ("x_own", 2),
    ("b_own", 1, 2), ("b_take", 0, 3), ("b_take", 0, 0), ("b_most", 0), ("b_own", 1, 1), ("b_pass", 0, 3),
    ("b_pass", 0, 0), ("x_own", 3), ("part", 0, 0), ("b_far", 0, 1), ("b_far", 0, 2), ("b_take", 1, 2), ("x_pass", 2),
    ("x_own", 4), ("b_own", 1, 3), ("part", 1, 0), ("b_take", 1, 1), ("x_pass", 3), ("pmid", 0, 1, 0),
    ("b_pass", 1, 2), ("b_far", 0, 0), ("b_pass", 1, 1), ("b_far", 0, 3), ("b_pass", 1, 0), ("x_pass", 4),
    ("b_rest", 0), ("part", 1, 1), ("part", 0, 1), ("pmid", 1, 1, 0), ("b_take", 1, 3), ("x_own", 5),
    ("b_pass", 1, 3), ("pmid", 0, 2, 0), ("product", 2), ("b_most", 1), ("part", 6, 0), ("x_own", 6), ("product", 3),
    ("pmid", 1, 1, 1), ("b_far", 1, 2), ("pmid", 0, 1, 1), ("product", 4), ("pmid", 1, 2, 0), ("b_far", 1, 1),
    ("b_far", 1, 0), ("b_far", 1, 3), ("mid", 2, 1), ("x_pass", 5), ("x_own", 7), ("x_own", 8), ("pmid", 0, 3, 0),
    ("pmid", 6, 1, 0), ("b_rest", 1), ("part", 6, 1), ("product", 8), ("x_pass", 6), ("mid", 3, 1), ("product", 7),
    ("mid", 4, 1), ("product", 10), ("pmid", 1, 2, 1), ("product", 9), ("mid", 8, 1), ("product", 5), ("x_pass", 7),
    ("x_pass", 8), ("mid", 2, 2), ("mid", 10, 1), ("product", 11), ("pmid", 0, 2, 1), ("pmid", 6, 2, 0),
    ("mid", 9, 1), ("mid", 7, 1), ("mid", 5, 1), ("pmid", 6, 1, 1), ("product", 12), ("mid", 11, 1), ("mid", 8, 2),
    ("product", 14), ("product", 13), ("mid", 7, 2), ("pmid", 6, 2, 1), ("mid", 10, 2), ("mid", 9, 2), ("mid", 12, 1),
    ("mid", 11, 2), ("pmid", 0, 3, 1), ("mid", 3, 2), ("mid", 14, 1), ("pmid", 6, 3, 1), ("mid", 13, 1),
    ("mid", 7, 3), ("mid", 9, 3), ("mid", 5, 2), ("mid", 8, 3), ("pmid", 6, 3, 0), ("mid", 10, 3), ("mid", 11, 3),
    ("mid", 4, 2), ("mid", 14, 2), ("mid", 12, 2), ("mid", 13, 2), ("mid", 3, 3), ("pmid", 1, 3, 0), ("last", 7),
    ("last", 9), ("last", 8), ("plast", 6), ("pmid", 1, 3, 1), ("mid", 5, 3), ("last", 11), ("mid", 2, 3),
    ("last", 10), ("mid", 4, 3), ("mid", 14, 3), ("mid", 12, 3), ("mid", 13, 3), ("last", 5), ("last", 4),
    ("last", 2), ("o_last", 1), ("plast", 1), ("o_last", 0), ("last", 3), ("o_last", 5), ("o_last", 2), ("last", 14),
    ("o_last", 3), ("last", 12), ("o_last", 4), ("plast", 0), ("last", 13),
)


def kernel(
    gate_hbm, up_hbm, grad_hbm, out_ref,
    gate_buf, up_buf, grad_buf, rows, turned, cols, prod, z_out, z_in, o_out, o_in,
    load_sem, grad_sem, x_send, x_recv, b_send, bx_recv, by_recv, bs_recv, z_send, z_recv, o_send, o_recv,
):
    tokens = grad_hbm.shape[0]
    node, local = lax.axis_index("node"), lax.axis_index("local")
    z, x = node // NX, node % NX
    y, core = local // NC, local % NC
    mine = y * NC + core

    def at(dz=0, dx=0, dy=0, dc=0):
        return {
            "node": lax.rem(z + dz + NZ, NZ) * NX + lax.rem(x + dx + NX, NX),
            "local": lax.rem(y + dy + NY, NY) * NC + lax.rem(core + dc, NC),
        }

    def remote(src, dst, send, recv, device):
        return pltpu.make_async_remote_copy(
            src_ref=src, dst_ref=dst, send_sem=send, recv_sem=recv, device_id=device, device_id_type=MESH
        )

    def arrived(ref, sem):
        remote(ref, ref, x_send, sem, at(dx=1)).wait_recv()

    def lanes(block):
        return pl.ds(pl.multiple_of(block * NB, NB), NB)

    def row_block(who):
        return pl.ds(pl.multiple_of(who * tokens, tokens), tokens)

    x_of = (x, lax.rem(x + NX - 1, NX), lax.rem(x + 1, NX), lax.rem(x + 2, NX))

    def piece(n, k, block):
        return cols.at[n, row_block(x_of[k]), lanes(block)]

    below = lax.rem(y + NY - 1, NY) * NC + core
    above = lax.rem(y + 1, NY) * NC + core
    across = lax.rem(y + 2, NY) * NC + core

    def b_send_to(n, k, dx):
        block = lax.rem(x + dx + 2 * n + NX, NX)
        remote(grad_buf.at[block], piece(n, 0, mine), b_send.at[0], bx_recv.at[n, k], at(dx=dx)).start()

    def b_near(n):
        b_send_to(n, 0, 1)
        b_send_to(n, 1, -1)

    def b_far2(n):
        b_send_to(n, 2, 2)

    def held(n, k, block, own):
        return grad_buf.at[lax.rem(x + 2 * n, NX)] if own and k == 0 else piece(n, k, block)

    def b_along(n, k, block, sem, dy, own=False):
        remote(held(n, k, block, own), piece(n, k, block), b_send.at[1], sem, at(dy=dy)).start()

    def b_over(n, k, block, part=0, own=False):
        remote(held(n, k, block, own), piece(n, k, block), b_send.at[2], bs_recv.at[n, part], at(dc=1)).start()

    def b_own(n, k):
        if k:
            with jax.named_scope(f"bx_{n}{k}"):
                arrived(grad_buf.at[0], bx_recv.at[n, k - 1])
        b_along(n, k, mine, by_recv.at[n, k, 0], 1, own=True)
        b_along(n, k, mine, by_recv.at[n, k, 0], -1, own=True)
        b_over(n, k, mine, own=True)

    def b_take(n, k):
        with jax.named_scope(f"by_{n}{k}"):
            arrived(rows.at[0, pl.ds(0, 2 * tokens), :], by_recv.at[n, k, 0])
        b_over(n, k, below)
        b_over(n, k, above)

    def b_pass(n, k):
        up = lax.rem(core + k, 2) == 0
        b_along(n, k, jnp.where(up, below, above), by_recv.at[n, k, 1], jnp.where(up, 1, -1))

    def b_far(n, k):
        with jax.named_scope(f"bf_{n}{k}"):
            arrived(grad_buf.at[0], by_recv.at[n, k, 1])
        b_over(n, k, across, 1)

    def b_most(n):
        with jax.named_scope(f"bm_{n}"):
            arrived(rows.at[pl.ds(0, 3)], bs_recv.at[n, 0])

    def b_rest(n):
        with jax.named_scope(f"br_{n}"):
            arrived(rows.at[0], bs_recv.at[n, 1])

    def rows_of(i, who):
        return rows.at[i, row_block(who), :]

    pair_step = 1 - 2 * lax.rem(x + core, 2)
    half = lax.rem(x - core + NX, NX) // 2

    def chunk_of(n):
        return 2 * n + half if n < PAIRS else n + PAIRS

    def step_of(n):
        return pair_step if n < PAIRS or n % 2 == 0 else -pair_step

    def x_own(n):
        mine_of, other = chunk_of(n), 2 * n + 1 - half if n < PAIRS else chunk_of(n)
        remote(rows_of(other, x), rows_of(other, x), x_send, x_recv.at[n, 0], at(dx=-step_of(n))).start()
        remote(rows_of(mine_of, x), rows_of(mine_of, x), x_send, x_recv.at[n, 1], at(dx=step_of(n))).start()

    def x_pass(n):
        with jax.named_scope("x_pass"):
            arrived(rows_of(0, x), x_recv.at[n, 0])
        block = rows_of(chunk_of(n), lax.rem(x - step_of(n) + NX, NX))
        remote(block, block, x_send, x_recv.at[n, 1], at(dx=step_of(n))).start()

    sign = 2 * core - 1

    def z_sem(u, sem):
        return z_recv.at[4 * u + 2 * sum(v < u for v in SPLIT) + sem]

    def z_move(u, slot, hop, sem):
        remote(z_out.at[u, slot], z_in.at[u, slot], z_send, z_sem(u, sem), at(dz=hop * sign)).start()

    def z_wait(u, count, sem):
        with jax.named_scope(f"z_{sem}"):
            arrived(z_in.at[u, pl.ds(0, count)], z_sem(u, sem))

    def block_at(offset):
        return lax.rem(z + offset * sign + NZ, NZ)

    def z_put(u, slot, offset, *added):
        value = prod[u, block_at(offset)]
        for other in added:
            value = value + z_in[u, other].astype(jnp.float32)
        z_out[u, slot] = value.astype(jnp.bfloat16)

    def is_quick(u):
        return u >= CHUNKS - QUICK

    def first(u):
        if is_quick(u):
            moves = ((0, 4, 2, 0), (4, -3, -2, 0), (1, 3, 1, 0), (5, -2, -1, 0), (3, 1, 1, 3))
        else:
            moves = ((0, 4, 1, 0), (4, -3, -1, 0))
        for slot, offset, hop, sem in moves:
            z_put(u, slot, offset)
            z_move(u, slot, hop, sem)

    def mid(u, s):
        z_wait(u, 2 if s < 3 else 1, s - 1)
        z_put(u, s, 4 - s, s - 1)
        z_move(u, s, 1, s if s < 3 else 3)
        if s < 3:
            z_put(u, 4 + s, s - 3, 3 + s)
            z_move(u, 4 + s, -1, s if s < 2 else 3)

    def qmid(u):
        z_wait(u, 4, 0)
        z_put(u, 2, 2, 0, 1)
        z_move(u, 2, 2, 3)
        z_put(u, 6, -1, 4, 5)
        z_move(u, 6, -1, 3)

    def if_part(offset, part, body):
        far = block_at(offset) // NC == lax.rem(y + 2, NY)
        pl.when(far if part else jnp.logical_not(far))(body)

    def pfirst(u, part):
        for slot, offset, hop, sem in ((0, 4, 1, 0), (4, -3, -1, 4)):
            def body(slot=slot, offset=offset, hop=hop, sem=sem):
                z_put(u, slot, offset)
                z_move(u, slot, hop, sem)
            if_part(offset, part, body)

    def pmid(u, s, part):
        def long():
            z_wait(u, 1, s - 1)
            z_put(u, s, 4 - s, s - 1)
            z_move(u, s, 1, s)

        def short():
            z_wait(u, 1, 3 + s)
            z_put(u, 4 + s, s - 3, 3 + s)
            z_move(u, 4 + s, -1, 4 + s if s < 2 else 3)

        if_part(4 - s, part, long)
        if s < 3:
            if_part(s - 3, part, short)

    def out_rows(chunk):
        return pl.ds(pl.multiple_of(chunk * MC, MC), MC)

    def last(u):
        added = (2, 3, 6) if is_quick(u) else (3, 6)
        z_wait(u, len(added), 3)
        value = prod[u, z]
        for other in added:
            value = value + z_in[u, other].astype(jnp.float32)
        value = value * (1.0 / (NZ * NX))
        n, second = UNITS[u]
        if second:
            o_out[n] = value.astype(jnp.bfloat16)
            remote(o_out.at[n], o_in.at[n], o_send, o_recv.at[n], at(dx=2)).start()
        else:
            out_ref[out_rows(chunk_of(n)), :] = value

    def o_last(n):
        with jax.named_scope("o"):
            arrived(o_in.at[0], o_recv.at[n])
        out_ref[out_rows(2 * n + 1 - half), :] = o_in[n].astype(jnp.float32)

    def rows_ready(u):
        n, second = UNITS[u]
        if not second:
            with jax.named_scope("x_last"):
                arrived(rows.at[0, pl.ds(0, 2 * tokens), :], x_recv.at[n, 1])
            turned[min(n, PAIRS)] = rows[chunk_of(n)].T

    def dot(u, place):
        n, second = UNITS[u]
        at_place = pl.ds(pl.multiple_of(place * NC * NB, NC * NB), NC * NB)
        value = jnp.dot(turned[min(n, PAIRS)], cols[second, :, at_place], preferred_element_type=jnp.float32)
        for i in range(NC):
            prod[u, NC * place + i] = value[:, i * NB : (i + 1) * NB]

    def product(u):
        rows_ready(u)
        with jax.named_scope("dot"):
            for place in range(NY):
                dot(u, place)
        first(u)

    def part(u, part):
        if part:
            dot(u, lax.rem(y + 2, NY))
        else:
            rows_ready(u)
            with jax.named_scope("dot"):
                for step in (0, 1, 3):
                    dot(u, lax.rem(y + step, NY))
        pfirst(u, part)

    def load(i):
        return (
            pltpu.make_async_copy(gate_hbm.at[:, lanes(i)], gate_buf.at[i], load_sem.at[i // LOADS]),
            pltpu.make_async_copy(up_hbm.at[:, lanes(i)], up_buf.at[i], load_sem.at[i // LOADS]),
        )

    def hide():
        def one(i, carry):
            gate = gate_buf[i].astype(jnp.float32)
            act = gate / (1.0 + jnp.exp(-gate))
            rows[i, row_block(x), :] = (act * up_buf[i].astype(jnp.float32)).astype(jnp.bfloat16)
            return carry

        for i in range(CHUNKS):
            for copy in load(i):
                copy.start()
        for n in range(2 if PAIRS else 1):
            cols[n, row_block(x), lanes(mine)] = grad_buf[lax.rem(x + 2 * n, NX)]
        with jax.named_scope("hide"):
            for group in range(CHUNKS // LOADS):
                both = gate_buf.at[pl.ds(0, 2 * LOADS)]
                pltpu.make_async_copy(both, both, load_sem.at[group]).wait()
                lax.fori_loop(group * LOADS, (group + 1) * LOADS, one, 0)

    partners = (
        at(dz=1), at(dz=-1), at(dx=1), at(dx=-1), at(dx=2), at(dy=1), at(dy=-1), at(dc=1),
    )
    if QUICK:
        partners += (at(dz=2), at(dz=-2))
    barrier = pltpu.get_barrier_semaphore()
    for device in partners:
        pl.semaphore_signal(barrier, inc=1, device_id=device, device_id_type=MESH)
    grad_copy = [
        pltpu.make_async_copy(grad_hbm.at[:, pl.ds(k * NB, NB)], grad_buf.at[k], grad_sem) for k in range(NX)
    ]
    for copy in grad_copy:
        copy.start()
    with jax.named_scope("grad"):
        pltpu.make_async_copy(grad_buf, grad_buf, grad_sem).wait()
    with jax.named_scope("barrier"):
        pl.semaphore_wait(barrier, len(partners))

    steps = {
        "b_near": b_near, "b_far2": b_far2, "b_own": b_own, "b_take": b_take, "b_pass": b_pass, "b_far": b_far,
        "b_most": b_most, "b_rest": b_rest, "part": part, "pmid": pmid, "plast": last,
        "hide": hide, "x_own": x_own, "x_pass": x_pass, "product": product, "mid": mid, "qmid": qmid, "last": last,
        "o_last": o_last,
    }
    for name, *arguments in ORDER:
        steps[name](*arguments)

    def sent(ref, sem):
        remote(ref, ref, sem, x_recv.at[0, 0], at(dx=1)).wait_send()

    with jax.named_scope("sent"):
        sent(rows.at[pl.ds(0, ITEMS), pl.ds(0, 3 * tokens), :], x_send)
        sets = 2 if PAIRS else 1
        sent(rows.at[pl.ds(0, sets), pl.ds(0, 3 * tokens), :], b_send.at[0])
        sent(rows.at[pl.ds(0, 3 * sets)], b_send.at[1])
        sent(rows.at[pl.ds(0, 4 * sets)], b_send.at[2])
        sent(z_out, z_send)
        if PAIRS:
            sent(o_out, o_send)


def solution(mesh):
    def shards(gate_pre, up_pre, out_grad):
        tokens, hidden = gate_pre.shape
        depth = NX * tokens
        dma = pltpu.SemaphoreType.DMA
        operands = [pltpu.with_memory_space_constraint(a, pltpu.HBM) for a in (gate_pre, up_pre, out_grad)]
        return pl.pallas_call(
            kernel,
            out_shape=jax.ShapeDtypeStruct((hidden, NB), jnp.float32),
            in_specs=[pl.BlockSpec(memory_space=pl.ANY)] * 3,
            out_specs=pl.BlockSpec(memory_space=pltpu.VMEM),
            scratch_shapes=[
                pltpu.VMEM((CHUNKS, tokens, MC), jnp.bfloat16),
                pltpu.VMEM((CHUNKS, tokens, MC), jnp.bfloat16),
                pltpu.VMEM((NX, tokens, NB), jnp.bfloat16),
                pltpu.VMEM((CHUNKS, depth, MC), jnp.bfloat16),
                pltpu.VMEM((PAIRS + 1, MC, depth), jnp.bfloat16),
                pltpu.VMEM((2, depth, NZ * NB), jnp.bfloat16),
                pltpu.VMEM((CHUNKS, NZ, MC, NB), jnp.float32),
                pltpu.VMEM((CHUNKS, 7, MC, NB), jnp.bfloat16),
                pltpu.VMEM((CHUNKS, 7, MC, NB), jnp.bfloat16),
                pltpu.VMEM((max(PAIRS, 1), MC, NB), jnp.bfloat16),
                pltpu.VMEM((max(PAIRS, 1), MC, NB), jnp.bfloat16),
                dma((CHUNKS // LOADS,)),
                dma,
                dma,
                dma((ITEMS, 2)),
                dma((3,)),
                dma((2, 3)),
                dma((2, NX, 2)),
                dma((2, 2)),
                dma,
                dma((4 * CHUNKS + 2 * len(SPLIT),)),
                dma,
                dma((max(PAIRS, 1),)),
            ],
            compiler_params=pltpu.CompilerParams(
                collective_id=0, has_side_effects=True, vmem_limit_bytes=VMEM_BYTES
            ),
        )(*operands)

    return jax.shard_map(
        shards,
        mesh=mesh,
        in_specs=(P("node", "local"), P("node", "local"), P("node", "local")),
        out_specs=P("local", "node"),
        check_vma=False,
    )
```
